512 devices in a mesh: harm: 32 (over z, x_hi), slab: 16 (over y, x_lo, core).
Axes of the slice: x: 4 (x_hi: 2, x_lo: 2; x = x_hi * 2 + x_lo), y: 4, z: 16, core: 2. Of those that a mesh axis runs over, the one named last changes fastest.
Arguments:
- harmonics: float32 [32, 2, 5, 32, 2048], P('harm', None, None, 'slab'), may hold values from -4 to 4
- mean_flow: float32 [5, 32, 2048], P(None, 'slab'), may hold values from 0.5 to 13.5
- freq_index: int32 [32], P('harm'), may hold values from 1 to 8
- wall_mask: int32 [32, 2048], P('slab'), may hold values 0 or 1
- jacobian_x: float32 [5, 5], replicated, may hold values from -2.5 to 2.5
- jacobian_y: float32 [5, 5], replicated, may hold values from -2.5 to 2.5
Outputs:
- mean_next: float32 [5, 32, 2048], P(None, 'slab')
- harmonics_next: float32 [32, 2, 5, 32, 2048], P('harm', None, None, 'slab')
The draws below stay inside these ranges and needn't reach their ends.
All inputs are finite; a program needn't handle non-finite values. No bound on the sum of `wall_mask` on one device may be relied on, other than what follows from the above.
Results may differ from the reference program's by a relative error of at most 0.00018.
Values sent between devices are 32-bit elements; how exact they have to be, the bound alone decides.
No kernel may reach another device: no remote copies, remote signals or barrier semaphores. Data moves between devices by JAX's collectives and lax.ppermute only.
A program may use at most 64 MiB of HBM per device.

```python
import jax
import jax.numpy as jnp
from jax import lax

NY = 32
NZ = 64
HARMONICS = 32
NX = 32


def draw_mean_flow(key, part):
    axial = jnp.arange(NX, dtype=jnp.float32) / (NX - 1)
    uniform_part = jax.random.uniform(key, (5, NX, NY * NZ), jnp.float32, 0.0, 1.0)
    profile = 1.0 + 2.0 * axial
    rough = 0.5 + uniform_part
    return profile[None, :, None] * rough


def touch_ends(drawn, own_key, low, largest):
    spot = [jax.random.randint(jax.random.fold_in(own_key, axis), (), 0, length) for axis, length in enumerate(drawn.shape)]
    widest = drawn.shape.index(max(drawn.shape))
    beside = spot[:widest] + [(spot[widest] + 1) % drawn.shape[widest]] + spot[widest + 1:]
    return drawn.at[tuple(spot)].set(low).at[tuple(beside)].set(largest)


def block_scale(own_key, extent, pieces, low, high):
    loudness, own = 1.0, jax.random.fold_in(own_key, 6)
    for axis_at, parts in pieces:
        draws = jnp.exp(jax.random.uniform(jax.random.fold_in(own, axis_at), (parts,), jnp.float32, low / len(pieces), high / len(pieces)))
        loudness = loudness * jnp.repeat(draws, extent[axis_at] // parts).reshape([-1 if axis == axis_at else 1 for axis in range(len(extent))])
    return loudness


def scatter_about(key, extent, scale, bound, cuts=(), kind=jnp.bfloat16):
    entries = scale * jax.random.normal(key, extent, jnp.float32)
    if cuts:
        entries = entries * block_scale(key, extent, cuts, -0.22, 0.18)
    return jnp.clip(entries, -bound, bound).astype(kind)


def setup_inputs(seed: int = 0) -> dict:
    splits = jax.random.split(jax.random.key(seed), 7)
    return {
        "harmonics": scatter_about(splits[0], (HARMONICS, 2, 5, NX, NY * NZ), 0.3, 4.0, ((0, 32), (3, 16)), jnp.float32),
        "mean_flow": draw_mean_flow(jax.random.fold_in(splits[6], 71), 0),
        "freq_index": touch_ends(jax.random.randint(splits[2], (HARMONICS,), 1, 9), jax.random.fold_in(splits[2], 1), 1, 8).astype(jnp.int32),
        "wall_mask": touch_ends((jax.random.randint(splits[3], (NX, NY * NZ), 0, 8) < 1).astype(jnp.int32), jax.random.fold_in(splits[3], 1), 0, 1),
        "jacobian_x": scatter_about(splits[4], (5, 5), 5 ** -0.5, 2.5, (), jnp.float32),
        "jacobian_y": scatter_about(splits[5], (5, 5), 5 ** -0.5, 2.5, (), jnp.float32),
    }


EPS_FOURTH = 0.05
COURANT = 0.9
OMEGA_BASE = 0.25
WALL_RATE = 2.0
HUB_RADIUS = 0.5
SECTION_RATES = (0.25, 1.0 / 3.0, 0.5, 1.0)
STRESS_PAIRS = ((1, 1), (1, 2), (1, 3), (2, 2), (2, 3), (3, 3), (4, 1), (4, 2), (4, 3))

def apply_matrix(matrix, values):
    return jnp.einsum('ab,...bxp->...axp', matrix, values, precision=lax.Precision.HIGHEST)

def diff_across(values):
    return (jnp.roll(values, -NZ, axis=-1) - jnp.roll(values, NZ, axis=-1)) * 0.5

def fourth_across(values):
    return jnp.roll(values, -2 * NZ, axis=-1) - 4.0 * jnp.roll(values, -NZ, axis=-1) + 6.0 * values - 4.0 * jnp.roll(values, NZ, axis=-1) + jnp.roll(values, 2 * NZ, axis=-1)

def diff_along(padded):
    return (padded[..., 3:-1, :] - padded[..., 1:-3, :]) * 0.5

def fourth_along(padded):
    return padded[..., 4:, :] - 4.0 * padded[..., 3:-1, :] + 6.0 * padded[..., 2:-2, :] - 4.0 * padded[..., 1:-3, :] + padded[..., :-4, :]

def harmonic_residual(harm_pad, momentum_pad, omega, wall_cells, jac_x, jac_y):
    center = harm_pad[..., 2:-2, :]
    flux_x = apply_matrix(jac_x, harm_pad * momentum_pad)
    flux_y = apply_matrix(jac_y, center)
    rotation = jnp.stack([center[..., 1, :, :, :], -center[..., 0, :, :, :]], axis=-4) * omega
    return rotation - diff_along(flux_x) - diff_across(flux_y) - EPS_FOURTH * (fourth_along(harm_pad) + fourth_across(center)) - WALL_RATE * wall_cells * center

def stresses(values):
    fields = []
    for first, second in STRESS_PAIRS:
        product = values[..., first, :, :] * values[..., second, :, :]
        fields.append(0.5 * lax.optimization_barrier(jnp.sum(product, axis=tuple(range(product.ndim - 2)))))
    return jnp.stack(fields, axis=0)

def forcing(stress_pad, radius):
    center = stress_pad[:, 1:-1, :]
    grad_x = (stress_pad[:, 2:, :] - stress_pad[:, :-2, :]) * 0.5
    grad_y = diff_across(center)
    first = -grad_x[0] - grad_y[1]
    second = -grad_x[1] - grad_y[3] - 2.0 * center[4] / radius
    third = -grad_x[2] - grad_y[4] + (center[3] - center[5]) / radius
    fourth = -grad_x[6] - grad_y[7] - center[8] / radius
    return jnp.stack([first, second, third, fourth], axis=0)

def mean_residual(mean_pad, forcing_terms, jac_x, jac_y):
    center = mean_pad[:, 2:-2, :]
    residual = -diff_along(apply_matrix(jac_x, mean_pad)) - diff_across(apply_matrix(jac_y, center)) - EPS_FOURTH * (fourth_along(mean_pad) + fourth_across(center))
    zeros_row = jnp.zeros_like(forcing_terms[:1])
    return residual + jnp.concatenate([zeros_row, forcing_terms], axis=0)

def reference(harmonics, mean_flow, freq_index, wall_mask, jacobian_x, jacobian_y):
    plane_count = mean_flow.shape[2]
    radius = HUB_RADIUS + ((jnp.arange(plane_count) % NZ).astype(jnp.float32) + 0.5) / NZ
    wall_cells = wall_mask.astype(jnp.float32)
    omegas = OMEGA_BASE * freq_index.astype(jnp.float32)
    speed_total = jnp.sum(mean_flow[1] * mean_flow[1])
    time_step = COURANT / (1.0 + jnp.sqrt(speed_total / (NX * NY * NZ)))
    harm_now, mean_now = (harmonics, mean_flow)
    for section_rate in SECTION_RATES:
        mean_pad = jnp.pad(mean_now, ((0, 0), (2, 2), (0, 0)))

        def single_residual(member):
            single, omega_one = member
            padded = jnp.pad(single, ((0, 0), (0, 0), (2, 2), (0, 0)))
            return harmonic_residual(padded, mean_pad[1], omega_one, wall_cells, jacobian_x, jacobian_y)
        harm_res = lax.map(single_residual, (harm_now, omegas))
        stress_pad = jnp.pad(stresses(harm_now), ((0, 0), (1, 1), (0, 0)))
        mean_res = mean_residual(mean_pad, forcing(stress_pad, radius), jacobian_x, jacobian_y)
        harm_now = harmonics + section_rate * time_step * harm_res
        mean_now = mean_flow + section_rate * time_step * mean_res
    return (mean_now, harm_now)
```

```python
import functools

import jax
import jax.numpy as jnp
from jax import lax
from jax.experimental import pallas as pl
from jax.experimental.pallas import tpu as pltpu
from jax.sharding import PartitionSpec as P

NZ = 64
EPS_FOURTH = 0.05
COURANT = 0.9
OMEGA_BASE = 0.25
WALL_RATE = 2.0
HUB_RADIUS = 0.5
SECTION_RATES = (0.25, 1.0 / 3.0, 0.5, 1.0)
STRESS_PAIRS = ((1, 1), (1, 2), (1, 3), (2, 2), (2, 3), (3, 3), (4, 1), (4, 2), (4, 3))

VARS = 5
CELLS = 2
C1 = 16
LANES = 128
H_ROWS = 2 * VARS * CELLS * C1
M_ROWS = VARS * CELLS * C1
W_ROWS = CELLS * C1


def h_row(part, var, cell):
    return ((part * VARS + var) * CELLS + cell) * C1


def m_row(var, cell):
    return (var * CELLS + cell) * C1


def pack_kernel(harm_ref, freq_ref, out_ref, rows_ref):
    for part in range(2):
        for var in range(VARS):
            for cell in range(CELLS):
                for c1 in range(C1):
                    row = h_row(part, var, cell) + c1
                    rows_ref[row : row + 1, :] = harm_ref[
                        0, part, var, cell : cell + 1, c1 * LANES : (c1 + 1) * LANES
                    ]
    omega = OMEGA_BASE * freq_ref[0].astype(jnp.float32)
    rows_ref[H_ROWS:, :] = jnp.full((rows_ref.shape[0] - H_ROWS, LANES), omega, jnp.float32)
    turned = rows_ref[...].T
    for j in range(32):
        out_ref[j, 0:2, :] = turned[2 * j : 2 * j + 2, :]
        out_ref[j, 2:4, :] = turned[NZ + 2 * j : NZ + 2 * j + 2, :]


def pack_mean(tiles):
    group = lax.broadcasted_iota(jnp.int32, (8, LANES), 1) // 4
    packed = jnp.zeros((8, LANES), jnp.float32)
    for i, tile in enumerate(tiles):
        for half in range(2):
            packed = jnp.where(group == 2 * i + half, tile[8 * half : 8 * half + 8, :], packed)
    return packed


def unpack_mean(packed):
    lane = lax.broadcasted_iota(jnp.int32, (8, LANES), 1) % 4
    tiles = []
    for i in range(VARS * CELLS):
        halves = [
            jnp.take_along_axis(packed, lane + 4 * (2 * i + half), axis=1) for half in range(2)
        ]
        tiles.append(jnp.concatenate(halves, axis=0))
    return tiles


def prepare_kernel(mean_ref, wall_ref, position_ref, mean_out, wall_out, packed_out, rows_ref):
    for cell in range(CELLS):
        for c1 in range(C1):
            cols = slice(c1 * LANES, (c1 + 1) * LANES)
            for var in range(VARS):
                row = m_row(var, cell) + c1
                rows_ref[row : row + 1, :] = mean_ref[var, cell : cell + 1, cols]
            row = M_ROWS + cell * C1 + c1
            rows_ref[row : row + 1, :] = wall_ref[cell : cell + 1, cols].astype(jnp.float32)
    lane = lax.broadcasted_iota(jnp.int32, (8, LANES), 1)
    source = ((lane // 2) % 2) * NZ + 2 * position_ref[0] + lane % 2
    for start in range(0, M_ROWS + W_ROWS, 8):
        picked = jnp.take_along_axis(rows_ref[start : start + 8, :], source, axis=1)
        if start < M_ROWS:
            mean_out[start : start + 8, :] = picked
        else:
            wall_out[start - M_ROWS : start - M_ROWS + 8, :] = picked
    packed_out[...] = pack_mean(
        [mean_out[i * C1 : (i + 1) * C1, :] for i in range(VARS * CELLS)]
    )


def unpack_kernel(arrived_ref, packed_ref, state_out, omega_out, rows_ref):
    for k in range(32):
        rows_ref[4 * k : 4 * k + 4, :] = arrived_ref[k]
    turned = rows_ref[...].T
    state_out[:H_ROWS, :] = turned[:H_ROWS, :]
    state_out[H_ROWS:, :] = packed_ref[...]
    omega_out[...] = turned[H_ROWS : H_ROWS + 8, :]


def section_kernel(
    own_ref, left_ref, right_ref, h0_ref, m0_ref, mean_ref, omega_ref, wall_ref, jac_ref,
    step_ref, radius_ref, *outs, rate, last
):
    lane = lax.broadcasted_iota(jnp.int32, (C1, LANES), 1)
    even = (lane // 2) % 2 == 0

    def up(tile):
        return pltpu.roll(tile, C1 - 1, 0)

    def down(tile):
        return pltpu.roll(tile, 1, 0)

    def beside(tile):
        swapped = jnp.where(even, pltpu.roll(tile, LANES - 2, 1), pltpu.roll(tile, 2, 1))
        return jnp.where(even, swapped, up(swapped)), jnp.where(even, down(swapped), swapped)

    def splat(ref, row):
        return jnp.broadcast_to(ref[row : row + 1, :], (C1, LANES))

    def apply_matrix(base, tiles):
        out = []
        for a in range(VARS):
            total = splat(jac_ref, base + VARS * a) * tiles[0]
            for b in range(1, VARS):
                total = total + splat(jac_ref, base + VARS * a + b) * tiles[b]
            out.append(total)
        return out

    def column(part, var):
        row = h_row(part, var, 0)
        return [
            ref[row + C1 * cell : row + C1 * (cell + 1), :]
            for ref in (left_ref, own_ref, right_ref)
            for cell in range(CELLS)
        ]

    omega = splat(omega_ref, 0)
    step = rate * splat(step_ref, 0)
    inv_radius = 1.0 / splat(radius_ref, 0)

    harm = [[column(part, var) for var in range(VARS)] for part in range(2)]
    left_mean = unpack_mean(left_ref[H_ROWS:, :])
    right_mean = unpack_mean(right_ref[H_ROWS:, :])
    mean = []
    for var in range(VARS):
        own_mean = [
            mean_ref[m_row(var, cell) : m_row(var, cell) + C1, :] for cell in range(CELLS)
        ]
        mean.append(
            left_mean[CELLS * var : CELLS * (var + 1)]
            + own_mean
            + right_mean[CELLS * var : CELLS * (var + 1)]
        )

    def smooth_parts(cells, at):
        center = cells[at]
        above, below = beside(center)
        diff_y = (above - below) * 0.5
        fourth = (
            (cells[at + 2] + cells[at - 2])
            + (up(center) + down(center))
            - 4.0 * ((cells[at + 1] + cells[at - 1]) + (above + below))
            + 12.0 * center
        )
        return diff_y, fourth

    harm_new = {}
    for cell in range(CELLS):
        at = 2 + cell
        wall = WALL_RATE * wall_ref[cell * C1 : (cell + 1) * C1, :]
        for part in range(2):
            diffs_x, diffs_y, fourths = [], [], []
            for var in range(VARS):
                cells = harm[part][var]
                diffs_x.append(
                    (mean[1][at + 1] * cells[at + 1] - mean[1][at - 1] * cells[at - 1]) * 0.5
                )
                diff_y, fourth = smooth_parts(cells, at)
                diffs_y.append(diff_y)
                fourths.append(fourth)
            flux_x = apply_matrix(0, diffs_x)
            flux_y = apply_matrix(VARS * VARS, diffs_y)
            for var in range(VARS):
                turned = omega * harm[1 - part][var][at]
                if part:
                    turned = -turned
                res = (
                    turned
                    - flux_x[var]
                    - flux_y[var]
                    - EPS_FOURTH * fourths[var]
                    - wall * harm[part][var][at]
                )
                row = h_row(part, var, cell)
                harm_new[part, var, cell] = h0_ref[row : row + C1, :] + step * res

    def stress(index, at):
        a, b = STRESS_PAIRS[index]
        return 0.5 * (harm[0][a][at] * harm[0][b][at] + harm[1][a][at] * harm[1][b][at])

    def total(tile):
        for shift in (4, 8, 16, 32, 64):
            tile = tile + pltpu.roll(tile, shift, 1)
        return jnp.take_along_axis(tile, lane % 4, axis=1)

    mean_new = {}
    for cell in range(CELLS):
        at = 2 + cell

        def grad_x(index):
            return (stress(index, at + 1) - stress(index, at - 1)) * 0.5

        def grad_y(tile):
            above, below = beside(tile)
            return (above - below) * 0.5

        s3, s4 = stress(3, at), stress(4, at)
        terms = [
            None,
            total(-grad_x(0) - grad_y(stress(1, at))),
            total(-grad_x(1) - grad_y(s3) - 2.0 * s4 * inv_radius),
            total(-grad_x(2) - grad_y(s4) + (s3 - stress(5, at)) * inv_radius),
            total(-grad_x(6) - grad_y(stress(7, at)) - stress(8, at) * inv_radius),
        ]
        diffs_x, diffs_y, fourths = [], [], []
        for var in range(VARS):
            cells = mean[var]
            diffs_x.append((cells[at + 1] - cells[at - 1]) * 0.5)
            diff_y, fourth = smooth_parts(cells, at)
            diffs_y.append(diff_y)
            fourths.append(fourth)
        flux_x = apply_matrix(0, diffs_x)
        flux_y = apply_matrix(VARS * VARS, diffs_y)
        for var in range(VARS):
            res = -flux_x[var] - flux_y[var] - EPS_FOURTH * fourths[var]
            if var:
                res = res + terms[var]
            row = m_row(var, cell)
            mean_new[var, cell] = m0_ref[row : row + C1, :] + step * res

    if last:
        out_ref, rows_ref = outs
        target, offset = rows_ref, H_ROWS
    else:
        state_out, mean_out = outs
        target, offset = state_out, None
    for (part, var, cell), tile in harm_new.items():
        row = h_row(part, var, cell)
        target[row : row + C1, :] = tile
    for (var, cell), tile in mean_new.items():
        row = m_row(var, cell)
        if last:
            target[offset + row : offset + row + C1, :] = tile
        else:
            mean_out[row : row + C1, :] = tile
    if last:
        spare = H_ROWS + M_ROWS
        rows_ref[spare:, :] = jnp.zeros((rows_ref.shape[0] - spare, LANES), jnp.float32)
        turned = rows_ref[...].T
        for k in range(32):
            out_ref[k] = turned[4 * k : 4 * k + 4, :]
    else:
        state_out[H_ROWS:, :] = pack_mean(
            [mean_new[var, cell] for var in range(VARS) for cell in range(CELLS)]
        )


def restore_kernel(arrived_ref, mean_out, harm_out, rows_ref):
    for j in range(32):
        rows_ref[2 * j : 2 * j + 2, :] = arrived_ref[j, 0:2, :]
        rows_ref[NZ + 2 * j : NZ + 2 * j + 2, :] = arrived_ref[j, 2:4, :]
    turned = rows_ref[...].T
    for var in range(VARS):
        for cell in range(CELLS):
            for c1 in range(C1):
                cols = slice(c1 * LANES, (c1 + 1) * LANES)
                for part in range(2):
                    row = h_row(part, var, cell) + c1
                    harm_out[0, part, var, cell : cell + 1, cols] = turned[row : row + 1, :]
                row = H_ROWS + m_row(var, cell) + c1
                mean_out[var, cell : cell + 1, cols] = turned[row : row + 1, :]


def f32(*shape):
    return jax.ShapeDtypeStruct(shape, jnp.float32)


VMEM = pl.BlockSpec(memory_space=pltpu.VMEM)
SMEM = pl.BlockSpec(memory_space=pltpu.SMEM)


def rows_scratch(*shape):
    return [pltpu.VMEM(shape, jnp.float32)]


def shards(harmonics, mean_flow, freq_index, wall_mask, jacobian_x, jacobian_y):
    plane_count = mean_flow.shape[2]
    slab_count = lax.axis_size("slab")
    position = lax.axis_index("harm")

    sends = pl.pallas_call(
        pack_kernel,
        out_shape=f32(32, 4, 384),
        in_specs=[VMEM, SMEM],
        out_specs=VMEM,
        scratch_shapes=rows_scratch(384, LANES),
        name="pack",
    )(harmonics, freq_index)
    arrived = lax.all_to_all(sends, "harm", 0, 0, tiled=True)

    speed = jnp.sum(mean_flow[1] * mean_flow[1])
    speeds = lax.all_to_all(
        jnp.broadcast_to(speed, (slab_count, 1, LANES)), "slab", 0, 0, tiled=True
    )
    speed_total = jnp.sum(speeds, axis=0)
    cell_count = CELLS * slab_count * plane_count
    step = COURANT / (1.0 + jnp.sqrt(speed_total / cell_count))

    mean_start, wall, packed = pl.pallas_call(
        prepare_kernel,
        out_shape=(f32(M_ROWS, LANES), f32(W_ROWS, LANES), f32(8, LANES)),
        in_specs=[VMEM, VMEM, SMEM],
        out_specs=(VMEM, VMEM, VMEM),
        scratch_shapes=rows_scratch(M_ROWS + W_ROWS, LANES),
        name="prepare",
    )(mean_flow, wall_mask, position.astype(jnp.int32).reshape(1))
    radial = 2 * position + jnp.arange(LANES) % 2
    radius = (HUB_RADIUS + (radial.astype(jnp.float32) + 0.5) / NZ).reshape(1, LANES)
    jac = jnp.concatenate([jacobian_x.reshape(-1, 1), jacobian_y.reshape(-1, 1)])
    jac = jnp.broadcast_to(jac, (2 * VARS * VARS, LANES))

    state, omega = pl.pallas_call(
        unpack_kernel,
        out_shape=(f32(H_ROWS + 8, LANES), f32(8, LANES)),
        in_specs=[VMEM, VMEM],
        out_specs=(VMEM, VMEM),
        scratch_shapes=rows_scratch(LANES, 384),
        name="unpack",
    )(arrived, packed)

    start, mean_now = state, mean_start
    for index, rate in enumerate(SECTION_RATES):
        last = index == len(SECTION_RATES) - 1
        left = lax.ppermute(state, "slab", [(i, i + 1) for i in range(slab_count - 1)])
        right = lax.ppermute(state, "slab", [(i + 1, i) for i in range(slab_count - 1)])
        if last:
            shapes, scratch = f32(32, 4, 512), rows_scratch(512, LANES)
            specs = VMEM
        else:
            shapes, scratch = (f32(H_ROWS + 8, LANES), f32(M_ROWS, LANES)), []
            specs = (VMEM, VMEM)
        result = pl.pallas_call(
            functools.partial(section_kernel, rate=rate, last=last),
            out_shape=shapes,
            in_specs=[VMEM] * 11,
            out_specs=specs,
            scratch_shapes=scratch,
            name=f"section{index}",
        )(state, left, right, start, mean_start, mean_now, omega, wall, jac, step, radius)
        if not last:
            state, mean_now = result
    back = lax.all_to_all(result, "harm", 0, 0, tiled=True)
    return pl.pallas_call(
        restore_kernel,
        out_shape=(f32(*mean_flow.shape), f32(*harmonics.shape)),
        in_specs=[VMEM],
        out_specs=(VMEM, VMEM),
        scratch_shapes=rows_scratch(LANES, 512),
        name="restore",
    )(back)


def solution(mesh):
    placed = (
        P("harm", None, None, "slab", None),
        P(None, "slab", None),
        P("harm"),
        P("slab", None),
        P(),
        P(),
    )
    return jax.shard_map(
        shards,
        mesh=mesh,
        in_specs=placed,
        out_specs=(P(None, "slab", None), P("harm", None, None, "slab", None)),
        check_vma=False,
    )
```

```python
import functools

import jax
import jax.numpy as jnp
from jax import lax
from jax.experimental import pallas as pl
from jax.experimental.pallas import tpu as pltpu
from jax.sharding import PartitionSpec as P

NZ = 64
EPS_FOURTH = 0.05
COURANT = 0.9
OMEGA_BASE = 0.25
WALL_RATE = 2.0
HUB_RADIUS = 0.5
SECTION_RATES = (0.25, 1.0 / 3.0, 0.5, 1.0)
STRESS_PAIRS = ((1, 1), (1, 2), (1, 3), (2, 2), (2, 3), (3, 3), (4, 1), (4, 2), (4, 3))

VARS = 5
CELLS = 2
C1 = 16
LANES = 128
H_ROWS = 2 * VARS * CELLS * C1
M_ROWS = VARS * CELLS * C1
W_ROWS = CELLS * C1


def h_row(part, var, cell):
    return ((part * VARS + var) * CELLS + cell) * C1


def m_row(var, cell):
    return (var * CELLS + cell) * C1


def pack_kernel(harm_ref, freq_ref, out_ref, rows_ref):
    for part in range(2):
        for var in range(VARS):
            for cell in range(CELLS):
                for c1 in range(C1):
                    row = h_row(part, var, cell) + c1
                    rows_ref[row : row + 1, :] = harm_ref[
                        0, part, var, cell : cell + 1, c1 * LANES : (c1 + 1) * LANES
                    ]
    omega = OMEGA_BASE * freq_ref[0].astype(jnp.float32)
    rows_ref[H_ROWS:, :] = jnp.full((rows_ref.shape[0] - H_ROWS, LANES), omega, jnp.float32)
    turned = rows_ref[...].T
    for j in range(32):
        out_ref[j, 0:2, :] = turned[2 * j : 2 * j + 2, :]
        out_ref[j, 2:4, :] = turned[NZ + 2 * j : NZ + 2 * j + 2, :]


def pack_mean(tiles):
    group = lax.broadcasted_iota(jnp.int32, (8, LANES), 1) // 4
    packed = jnp.zeros((8, LANES), jnp.float32)
    for i, tile in enumerate(tiles):
        for half in range(2):
            packed = jnp.where(group == 2 * i + half, tile[8 * half : 8 * half + 8, :], packed)
    return packed


def unpack_mean(packed):
    lane = lax.broadcasted_iota(jnp.int32, (8, LANES), 1) % 4
    tiles = []
    for i in range(VARS * CELLS):
        halves = [
            jnp.take_along_axis(packed, lane + 4 * (2 * i + half), axis=1) for half in range(2)
        ]
        tiles.append(jnp.concatenate(halves, axis=0))
    return tiles


def prepare_kernel(
    mean_ref, wall_ref, position_ref, mean_out, wall_out, packed_out, speed_out, rows_ref
):
    for cell in range(CELLS):
        for c1 in range(C1):
            cols = slice(c1 * LANES, (c1 + 1) * LANES)
            for var in range(VARS):
                row = m_row(var, cell) + c1
                rows_ref[row : row + 1, :] = mean_ref[var, cell : cell + 1, cols]
            row = M_ROWS + cell * C1 + c1
            rows_ref[row : row + 1, :] = wall_ref[cell : cell + 1, cols].astype(jnp.float32)
    lane = lax.broadcasted_iota(jnp.int32, (8, LANES), 1)
    source = ((lane // 2) % 2) * NZ + 2 * position_ref[0] + lane % 2
    for start in range(0, M_ROWS + W_ROWS, 8):
        picked = jnp.take_along_axis(rows_ref[start : start + 8, :], source, axis=1)
        if start < M_ROWS:
            mean_out[start : start + 8, :] = picked
        else:
            wall_out[start - M_ROWS : start - M_ROWS + 8, :] = picked
    momentum = rows_ref[m_row(1, 0) : m_row(2, 0), :]
    speed_out[...] = jnp.full((8, LANES), jnp.sum(momentum * momentum), jnp.float32)
    packed_out[...] = pack_mean(
        [mean_out[i * C1 : (i + 1) * C1, :] for i in range(VARS * CELLS)]
    )


def unpack_kernel(arrived_ref, packed_ref, state_out, omega_out, rows_ref):
    for k in range(32):
        rows_ref[4 * k : 4 * k + 4, :] = arrived_ref[k]
    turned = rows_ref[...].T
    state_out[:H_ROWS, :] = turned[:H_ROWS, :]
    state_out[H_ROWS:, :] = packed_ref[...]
    omega_out[...] = turned[H_ROWS : H_ROWS + 8, :]


def section_kernel(
    own_ref, left_ref, right_ref, h0_ref, m0_ref, mean_ref, omega_ref, wall_ref, jac_ref,
    step_ref, radius_ref, *outs, rate, last
):
    lane = lax.broadcasted_iota(jnp.int32, (C1, LANES), 1)
    even = (lane // 2) % 2 == 0

    def up(tile):
        return pltpu.roll(tile, C1 - 1, 0)

    def down(tile):
        return pltpu.roll(tile, 1, 0)

    def beside(tile):
        swapped = jnp.where(even, pltpu.roll(tile, LANES - 2, 1), pltpu.roll(tile, 2, 1))
        return jnp.where(even, swapped, up(swapped)), jnp.where(even, down(swapped), swapped)

    def splat(ref, row):
        return jnp.broadcast_to(ref[row : row + 1, :], (C1, LANES))

    def apply_matrix(base, tiles):
        out = []
        for a in range(VARS):
            total = splat(jac_ref, base + VARS * a) * tiles[0]
            for b in range(1, VARS):
                total = total + splat(jac_ref, base + VARS * a + b) * tiles[b]
            out.append(total)
        return out

    def column(part, var):
        row = h_row(part, var, 0)
        return [
            ref[row + C1 * cell : row + C1 * (cell + 1), :]
            for ref in (left_ref, own_ref, right_ref)
            for cell in range(CELLS)
        ]

    omega = splat(omega_ref, 0)
    step = rate * splat(step_ref, 0)
    inv_radius = 1.0 / splat(radius_ref, 0)

    harm = [[column(part, var) for var in range(VARS)] for part in range(2)]
    left_mean = unpack_mean(left_ref[H_ROWS:, :])
    right_mean = unpack_mean(right_ref[H_ROWS:, :])
    mean = []
    for var in range(VARS):
        own_mean = [
            mean_ref[m_row(var, cell) : m_row(var, cell) + C1, :] for cell in range(CELLS)
        ]
        mean.append(
            left_mean[CELLS * var : CELLS * (var + 1)]
            + own_mean
            + right_mean[CELLS * var : CELLS * (var + 1)]
        )

    def smooth_parts(cells, at):
        center = cells[at]
        above, below = beside(center)
        diff_y = (above - below) * 0.5
        fourth = (
            (cells[at + 2] + cells[at - 2])
            + (up(center) + down(center))
            - 4.0 * ((cells[at + 1] + cells[at - 1]) + (above + below))
            + 12.0 * center
        )
        return diff_y, fourth

    harm_new = {}
    for cell in range(CELLS):
        at = 2 + cell
        wall = WALL_RATE * wall_ref[cell * C1 : (cell + 1) * C1, :]
        for part in range(2):
            diffs_x, diffs_y, fourths = [], [], []
            for var in range(VARS):
                cells = harm[part][var]
                diffs_x.append(
                    (mean[1][at + 1] * cells[at + 1] - mean[1][at - 1] * cells[at - 1]) * 0.5
                )
                diff_y, fourth = smooth_parts(cells, at)
                diffs_y.append(diff_y)
                fourths.append(fourth)
            flux_x = apply_matrix(0, diffs_x)
            flux_y = apply_matrix(VARS * VARS, diffs_y)
            for var in range(VARS):
                turned = omega * harm[1 - part][var][at]
                if part:
                    turned = -turned
                res = (
                    turned
                    - flux_x[var]
                    - flux_y[var]
                    - EPS_FOURTH * fourths[var]
                    - wall * harm[part][var][at]
                )
                row = h_row(part, var, cell)
                harm_new[part, var, cell] = h0_ref[row : row + C1, :] + step * res

    def stress(index, at):
        a, b = STRESS_PAIRS[index]
        return 0.5 * (harm[0][a][at] * harm[0][b][at] + harm[1][a][at] * harm[1][b][at])

    def total(tile):
        for shift in (4, 8, 16, 32, 64):
            tile = tile + pltpu.roll(tile, shift, 1)
        return jnp.take_along_axis(tile, lane % 4, axis=1)

    mean_new = {}
    for cell in range(CELLS):
        at = 2 + cell

        def grad_x(index):
            return (stress(index, at + 1) - stress(index, at - 1)) * 0.5

        def grad_y(tile):
            above, below = beside(tile)
            return (above - below) * 0.5

        s3, s4 = stress(3, at), stress(4, at)
        terms = [
            None,
            total(-grad_x(0) - grad_y(stress(1, at))),
            total(-grad_x(1) - grad_y(s3) - 2.0 * s4 * inv_radius),
            total(-grad_x(2) - grad_y(s4) + (s3 - stress(5, at)) * inv_radius),
            total(-grad_x(6) - grad_y(stress(7, at)) - stress(8, at) * inv_radius),
        ]
        diffs_x, diffs_y, fourths = [], [], []
        for var in range(VARS):
            cells = mean[var]
            diffs_x.append((cells[at + 1] - cells[at - 1]) * 0.5)
            diff_y, fourth = smooth_parts(cells, at)
            diffs_y.append(diff_y)
            fourths.append(fourth)
        flux_x = apply_matrix(0, diffs_x)
        flux_y = apply_matrix(VARS * VARS, diffs_y)
        for var in range(VARS):
            res = -flux_x[var] - flux_y[var] - EPS_FOURTH * fourths[var]
            if var:
                res = res + terms[var]
            row = m_row(var, cell)
            mean_new[var, cell] = m0_ref[row : row + C1, :] + step * res

    if last:
        out_ref, rows_ref = outs
        target, offset = rows_ref, H_ROWS
    else:
        state_out, mean_out = outs
        target, offset = state_out, None
    for (part, var, cell), tile in harm_new.items():
        row = h_row(part, var, cell)
        target[row : row + C1, :] = tile
    for (var, cell), tile in mean_new.items():
        row = m_row(var, cell)
        if last:
            target[offset + row : offset + row + C1, :] = tile
        else:
            mean_out[row : row + C1, :] = tile
    if last:
        spare = H_ROWS + M_ROWS
        rows_ref[spare:, :] = jnp.zeros((rows_ref.shape[0] - spare, LANES), jnp.float32)
        turned = rows_ref[...].T
        for k in range(32):
            out_ref[k] = turned[4 * k : 4 * k + 4, :]
    else:
        state_out[H_ROWS:, :] = pack_mean(
            [mean_new[var, cell] for var in range(VARS) for cell in range(CELLS)]
        )


def restore_kernel(arrived_ref, mean_out, harm_out, rows_ref):
    for j in range(32):
        rows_ref[2 * j : 2 * j + 2, :] = arrived_ref[j, 0:2, :]
        rows_ref[NZ + 2 * j : NZ + 2 * j + 2, :] = arrived_ref[j, 2:4, :]
    turned = rows_ref[...].T
    for var in range(VARS):
        for cell in range(CELLS):
            for c1 in range(C1):
                cols = slice(c1 * LANES, (c1 + 1) * LANES)
                for part in range(2):
                    row = h_row(part, var, cell) + c1
                    harm_out[0, part, var, cell : cell + 1, cols] = turned[row : row + 1, :]
                row = H_ROWS + m_row(var, cell) + c1
                mean_out[var, cell : cell + 1, cols] = turned[row : row + 1, :]


def f32(*shape):
    return jax.ShapeDtypeStruct(shape, jnp.float32)


def kept(*shape):
    return pltpu.VMEM(shape, jnp.float32)


def held(*arrays):
    return [pltpu.with_memory_space_constraint(array, pltpu.VMEM) for array in arrays]


def summed(value, axis):
    count = lax.axis_size(axis)
    reach = 1
    while reach < count:
        value = value + lax.ppermute(value, axis, [(i, i ^ reach) for i in range(count)])
        reach *= 2
    return value


VMEM = pl.BlockSpec(memory_space=pltpu.VMEM)
SMEM = pl.BlockSpec(memory_space=pltpu.SMEM)


def rows_scratch(*shape):
    return [pltpu.VMEM(shape, jnp.float32)]


def shards(harmonics, mean_flow, freq_index, wall_mask, jacobian_x, jacobian_y):
    plane_count = mean_flow.shape[2]
    slab_count = lax.axis_size("slab")
    position = lax.axis_index("harm")

    sends = pl.pallas_call(
        pack_kernel,
        out_shape=kept(32, 4, 384),
        in_specs=[VMEM, SMEM],
        out_specs=VMEM,
        scratch_shapes=rows_scratch(384, LANES),
        name="pack",
    )(harmonics, freq_index)
    sends, mean_flow, wall_mask, jacobian_x, jacobian_y = lax.optimization_barrier(
        (sends, mean_flow, wall_mask, jacobian_x, jacobian_y)
    )
    arrived = lax.all_to_all(sends, "harm", 0, 0, tiled=True)

    mean_start, wall, packed, speed = pl.pallas_call(
        prepare_kernel,
        out_shape=(kept(M_ROWS, LANES), kept(W_ROWS, LANES), kept(8, LANES), kept(8, LANES)),
        in_specs=[VMEM, VMEM, SMEM],
        out_specs=(VMEM,) * 4,
        scratch_shapes=rows_scratch(M_ROWS + W_ROWS, LANES),
        name="prepare",
    )(mean_flow, wall_mask, position.astype(jnp.int32).reshape(1))
    cell_count = CELLS * slab_count * plane_count
    step = COURANT / (1.0 + jnp.sqrt(summed(speed, "slab") / cell_count))
    radial = 2 * position + jnp.arange(LANES) % 2
    radius = (HUB_RADIUS + (radial.astype(jnp.float32) + 0.5) / NZ).reshape(1, LANES)
    jac = jnp.concatenate([jacobian_x.reshape(-1, 1), jacobian_y.reshape(-1, 1)])
    jac = jnp.broadcast_to(jac, (2 * VARS * VARS, LANES))

    state, omega = pl.pallas_call(
        unpack_kernel,
        out_shape=(kept(H_ROWS + 8, LANES), kept(8, LANES)),
        in_specs=[VMEM, VMEM],
        out_specs=(VMEM, VMEM),
        scratch_shapes=rows_scratch(LANES, 384),
        name="unpack",
    )(*held(arrived, packed))

    start, mean_now = state, mean_start
    for index, rate in enumerate(SECTION_RATES):
        last = index == len(SECTION_RATES) - 1
        left = lax.ppermute(state, "slab", [(i, i + 1) for i in range(slab_count - 1)])
        right = lax.ppermute(state, "slab", [(i + 1, i) for i in range(slab_count - 1)])
        if last:
            shapes, scratch = kept(32, 4, 512), rows_scratch(512, LANES)
            specs = VMEM
        else:
            shapes, scratch = (kept(H_ROWS + 8, LANES), kept(M_ROWS, LANES)), []
            specs = (VMEM, VMEM)
        result = pl.pallas_call(
            functools.partial(section_kernel, rate=rate, last=last),
            out_shape=shapes,
            in_specs=[VMEM] * 11,
            out_specs=specs,
            scratch_shapes=scratch,
            name=f"section{index}",
        )(
            *held(
                state, left, right, start, mean_start, mean_now, omega, wall, jac, step, radius
            )
        )
        if not last:
            state, mean_now = result
    back = lax.all_to_all(result, "harm", 0, 0, tiled=True)
    return pl.pallas_call(
        restore_kernel,
        out_shape=(f32(*mean_flow.shape), f32(*harmonics.shape)),
        in_specs=[VMEM],
        out_specs=(VMEM, VMEM),
        scratch_shapes=rows_scratch(LANES, 512),
        name="restore",
    )(*held(back))


def solution(mesh):
    placed = (
        P("harm", None, None, "slab", None),
        P(None, "slab", None),
        P("harm"),
        P("slab", None),
        P(),
        P(),
    )
    return jax.shard_map(
        shards,
        mesh=mesh,
        in_specs=placed,
        out_specs=(P(None, "slab", None), P("harm", None, None, "slab", None)),
        check_vma=False,
    )
```

```python
import functools

import jax
import jax.numpy as jnp
from jax import lax
from jax.experimental import pallas as pl
from jax.experimental.pallas import tpu as pltpu
from jax.sharding import PartitionSpec as P


NZ = 64
EPS_FOURTH = 0.05
COURANT = 0.9
OMEGA_BASE = 0.25
WALL_RATE = 2.0
HUB_RADIUS = 0.5
SECTION_RATES = (0.25, 1.0 / 3.0, 0.5, 1.0)
STRESS_PAIRS = ((1, 1), (1, 2), (1, 3), (2, 2), (2, 3), (3, 3), (4, 1), (4, 2), (4, 3))

VARS = 5
CELLS = 2
C1 = 16
LANES = 128
H_ROWS = 2 * VARS * CELLS * C1
M_ROWS = VARS * CELLS * C1
W_ROWS = CELLS * C1


def h_row(part, var, cell):
    return ((part * VARS + var) * CELLS + cell) * C1


def m_row(var, cell):
    return (var * CELLS + cell) * C1


def pack_kernel(harm_ref, freq_ref, out_ref, token_ref, rows_ref):
    for part in range(2):
        for var in range(VARS):
            for cell in range(CELLS):
                for c1 in range(C1):
                    row = h_row(part, var, cell) + c1
                    rows_ref[row : row + 1, :] = harm_ref[
                        0, part, var, cell : cell + 1, c1 * LANES : (c1 + 1) * LANES
                    ]
    omega = OMEGA_BASE * freq_ref[0].astype(jnp.float32)
    rows_ref[H_ROWS:, :] = jnp.full((rows_ref.shape[0] - H_ROWS, LANES), omega, jnp.float32)
    token_ref[...] = jnp.full((8, LANES), omega, jnp.float32)
    turned = rows_ref[...].T
    for j in range(32):
        out_ref[j, 0:2, :] = turned[2 * j : 2 * j + 2, :]
        out_ref[j, 2:4, :] = turned[NZ + 2 * j : NZ + 2 * j + 2, :]


def pack_mean(tiles):
    group = lax.broadcasted_iota(jnp.int32, (8, LANES), 1) // 4
    packed = jnp.zeros((8, LANES), jnp.float32)
    for i, tile in enumerate(tiles):
        for half in range(2):
            packed = jnp.where(group == 2 * i + half, tile[8 * half : 8 * half + 8, :], packed)
    return packed


def unpack_mean(packed):
    lane = lax.broadcasted_iota(jnp.int32, (8, LANES), 1) % 4
    tiles = []
    for i in range(VARS * CELLS):
        halves = [
            jnp.take_along_axis(packed, lane + 4 * (2 * i + half), axis=1) for half in range(2)
        ]
        tiles.append(jnp.concatenate(halves, axis=0))
    return tiles


def prepare_kernel(
    mean_ref, wall_ref, position_ref, token_ref, mean_out, wall_out, packed_out, speed_out, rows_ref
):
    del token_ref
    for cell in range(CELLS):
        for c1 in range(C1):
            cols = slice(c1 * LANES, (c1 + 1) * LANES)
            for var in range(VARS):
                row = m_row(var, cell) + c1
                rows_ref[row : row + 1, :] = mean_ref[var, cell : cell + 1, cols]
            row = M_ROWS + cell * C1 + c1
            rows_ref[row : row + 1, :] = wall_ref[cell : cell + 1, cols].astype(jnp.float32)
    lane = lax.broadcasted_iota(jnp.int32, (8, LANES), 1)
    source = ((lane // 2) % 2) * NZ + 2 * position_ref[0] + lane % 2
    for start in range(0, M_ROWS + W_ROWS, 8):
        picked = jnp.take_along_axis(rows_ref[start : start + 8, :], source, axis=1)
        if start < M_ROWS:
            mean_out[start : start + 8, :] = picked
        else:
            wall_out[start - M_ROWS : start - M_ROWS + 8, :] = picked
    momentum = rows_ref[m_row(1, 0) : m_row(2, 0), :]
    speed_out[...] = jnp.full(speed_out.shape, jnp.sum(momentum * momentum), jnp.float32)
    packed_out[...] = pack_mean(
        [mean_out[i * C1 : (i + 1) * C1, :] for i in range(VARS * CELLS)]
    )


def unpack_kernel(arrived_ref, packed_ref, speed_ref, state_out, omega_out, speed_out, rows_ref):
    speed_out[...] = speed_ref[...]
    for k in range(32):
        rows_ref[4 * k : 4 * k + 4, :] = arrived_ref[k]
    turned = rows_ref[...].T
    state_out[:H_ROWS, :] = turned[:H_ROWS, :]
    state_out[H_ROWS:, :] = packed_ref[...]
    omega_out[...] = turned[H_ROWS : H_ROWS + 8, :]


def section_kernel(*refs, stage, cell_count):
    last = stage == len(SECTION_RATES) - 1
    own_ref, left_ref, right_ref, mean_ref, omega_ref, wall_ref, jac_ref, radius_ref = refs[:8]
    refs = refs[8:]
    if stage == 0:
        outs = refs
    elif stage == 1:
        speed_ref, own_res, left_res, right_res, mean_res, *outs = refs
        h0_ref, m0_ref = own_ref, mean_ref
    else:
        speed_ref, h0_ref, m0_ref, *outs = refs
    lane = lax.broadcasted_iota(jnp.int32, (C1, LANES), 1)
    even = (lane // 2) % 2 == 0

    def up(tile):
        return pltpu.roll(tile, C1 - 1, 0)

    def down(tile):
        return pltpu.roll(tile, 1, 0)

    def beside(tile):
        swapped = jnp.where(even, pltpu.roll(tile, LANES - 2, 1), pltpu.roll(tile, 2, 1))
        return jnp.where(even, swapped, up(swapped)), jnp.where(even, down(swapped), swapped)

    def splat(ref, row):
        return jnp.broadcast_to(ref[row : row + 1, :], (C1, LANES))

    def apply_matrix(base, tiles):
        out = []
        for a in range(VARS):
            total = splat(jac_ref, base + VARS * a) * tiles[0]
            for b in range(1, VARS):
                total = total + splat(jac_ref, base + VARS * a + b) * tiles[b]
            out.append(total)
        return out

    omega = splat(omega_ref, 0)
    if stage:
        speed_total = jnp.sum(speed_ref[...], axis=0)
        time_step = COURANT / (1.0 + jnp.sqrt(speed_total / cell_count))
        time_step = jnp.broadcast_to(time_step, (C1, LANES))
        step = SECTION_RATES[stage] * time_step
    blocks = [(left_ref, None), (own_ref, None), (right_ref, None)]
    mean_block = (mean_ref, None)
    if stage == 1:
        first = SECTION_RATES[0] * time_step
        blocks = [(left_ref, left_res), (own_ref, own_res), (right_ref, right_res)]
        mean_block = (mean_ref, mean_res)

    def load(block, row, count=C1):
        base, residual = block
        value = base[row : row + count, :]
        if residual is not None:
            value = value + first[:count] * residual[row : row + count, :]
        return value

    def column(part, var):
        row = h_row(part, var, 0)
        return [load(block, row + C1 * cell) for block in blocks for cell in range(CELLS)]

    inv_radius = 1.0 / splat(radius_ref, 0)

    harm = [[column(part, var) for var in range(VARS)] for part in range(2)]
    left_mean = unpack_mean(load(blocks[0], H_ROWS, 8))
    right_mean = unpack_mean(load(blocks[2], H_ROWS, 8))
    mean = []
    for var in range(VARS):
        own_mean = [load(mean_block, m_row(var, cell)) for cell in range(CELLS)]
        mean.append(
            left_mean[CELLS * var : CELLS * (var + 1)]
            + own_mean
            + right_mean[CELLS * var : CELLS * (var + 1)]
        )

    def smooth_parts(cells, at):
        center = cells[at]
        above, below = beside(center)
        diff_y = (above - below) * 0.5
        fourth = (
            (cells[at + 2] + cells[at - 2])
            + (up(center) + down(center))
            - 4.0 * ((cells[at + 1] + cells[at - 1]) + (above + below))
            + 12.0 * center
        )
        return diff_y, fourth

    harm_new = {}
    for cell in range(CELLS):
        at = 2 + cell
        wall = WALL_RATE * wall_ref[cell * C1 : (cell + 1) * C1, :]
        for part in range(2):
            diffs_x, diffs_y, fourths = [], [], []
            for var in range(VARS):
                cells = harm[part][var]
                diffs_x.append(
                    (mean[1][at + 1] * cells[at + 1] - mean[1][at - 1] * cells[at - 1]) * 0.5
                )
                diff_y, fourth = smooth_parts(cells, at)
                diffs_y.append(diff_y)
                fourths.append(fourth)
            flux_x = apply_matrix(0, diffs_x)
            flux_y = apply_matrix(VARS * VARS, diffs_y)
            for var in range(VARS):
                turned = omega * harm[1 - part][var][at]
                if part:
                    turned = -turned
                res = (
                    turned
                    - flux_x[var]
                    - flux_y[var]
                    - EPS_FOURTH * fourths[var]
                    - wall * harm[part][var][at]
                )
                row = h_row(part, var, cell)
                if stage:
                    res = h0_ref[row : row + C1, :] + step * res
                harm_new[part, var, cell] = res

    def stress(index, at):
        a, b = STRESS_PAIRS[index]
        return 0.5 * (harm[0][a][at] * harm[0][b][at] + harm[1][a][at] * harm[1][b][at])

    def total(tile):
        for shift in (4, 8, 16, 32, 64):
            tile = tile + pltpu.roll(tile, shift, 1)
        return jnp.take_along_axis(tile, lane % 4, axis=1)

    mean_new = {}
    for cell in range(CELLS):
        at = 2 + cell

        def grad_x(index):
            return (stress(index, at + 1) - stress(index, at - 1)) * 0.5

        def grad_y(tile):
            above, below = beside(tile)
            return (above - below) * 0.5

        s3, s4 = stress(3, at), stress(4, at)
        terms = [
            None,
            total(-grad_x(0) - grad_y(stress(1, at))),
            total(-grad_x(1) - grad_y(s3) - 2.0 * s4 * inv_radius),
            total(-grad_x(2) - grad_y(s4) + (s3 - stress(5, at)) * inv_radius),
            total(-grad_x(6) - grad_y(stress(7, at)) - stress(8, at) * inv_radius),
        ]
        diffs_x, diffs_y, fourths = [], [], []
        for var in range(VARS):
            cells = mean[var]
            diffs_x.append((cells[at + 1] - cells[at - 1]) * 0.5)
            diff_y, fourth = smooth_parts(cells, at)
            diffs_y.append(diff_y)
            fourths.append(fourth)
        flux_x = apply_matrix(0, diffs_x)
        flux_y = apply_matrix(VARS * VARS, diffs_y)
        for var in range(VARS):
            res = -flux_x[var] - flux_y[var] - EPS_FOURTH * fourths[var]
            if var:
                res = res + terms[var]
            row = m_row(var, cell)
            if stage:
                res = m0_ref[row : row + C1, :] + step * res
            mean_new[var, cell] = res

    if last:
        out_ref, rows_ref = outs
        target, offset = rows_ref, H_ROWS
    else:
        state_out, mean_out = outs
        target, offset = state_out, None
    for (part, var, cell), tile in harm_new.items():
        row = h_row(part, var, cell)
        target[row : row + C1, :] = tile
    for (var, cell), tile in mean_new.items():
        row = m_row(var, cell)
        if last:
            target[offset + row : offset + row + C1, :] = tile
        else:
            mean_out[row : row + C1, :] = tile
    if last:
        spare = H_ROWS + M_ROWS
        rows_ref[spare:, :] = jnp.zeros((rows_ref.shape[0] - spare, LANES), jnp.float32)
        turned = rows_ref[...].T
        for k in range(32):
            out_ref[k] = turned[4 * k : 4 * k + 4, :]
    else:
        state_out[H_ROWS:, :] = pack_mean(
            [mean_new[var, cell] for var in range(VARS) for cell in range(CELLS)]
        )


def restore_kernel(arrived_ref, mean_out, harm_out, rows_ref):
    for j in range(32):
        rows_ref[2 * j : 2 * j + 2, :] = arrived_ref[j, 0:2, :]
        rows_ref[NZ + 2 * j : NZ + 2 * j + 2, :] = arrived_ref[j, 2:4, :]
    turned = rows_ref[...].T
    for var in range(VARS):
        for cell in range(CELLS):
            for c1 in range(C1):
                cols = slice(c1 * LANES, (c1 + 1) * LANES)
                for part in range(2):
                    row = h_row(part, var, cell) + c1
                    harm_out[0, part, var, cell : cell + 1, cols] = turned[row : row + 1, :]
                row = H_ROWS + m_row(var, cell) + c1
                mean_out[var, cell : cell + 1, cols] = turned[row : row + 1, :]


def f32(*shape):
    return jax.ShapeDtypeStruct(shape, jnp.float32)


def kept(*shape):
    return pltpu.VMEM(shape, jnp.float32)


def held(*arrays):
    return [pltpu.with_memory_space_constraint(array, pltpu.VMEM) for array in arrays]


VMEM = pl.BlockSpec(memory_space=pltpu.VMEM)
SMEM = pl.BlockSpec(memory_space=pltpu.SMEM)


def rows_scratch(*shape):
    return [pltpu.VMEM(shape, jnp.float32)]


def shards(harmonics, mean_flow, freq_index, wall_mask, jacobian_x, jacobian_y):
    plane_count = mean_flow.shape[2]
    slab_count = lax.axis_size("slab")
    position = lax.axis_index("harm")

    sends, token = pl.pallas_call(
        pack_kernel,
        out_shape=(kept(32, 4, 384), kept(8, LANES)),
        in_specs=[VMEM, SMEM],
        out_specs=(VMEM, VMEM),
        scratch_shapes=rows_scratch(384, LANES),
        name="pack",
    )(harmonics, freq_index)
    arrived = lax.all_to_all(sends, "harm", 0, 0, tiled=True)

    mean_start, wall, packed, speed = pl.pallas_call(
        prepare_kernel,
        out_shape=(
            kept(M_ROWS, LANES),
            kept(W_ROWS, LANES),
            kept(8, LANES),
            kept(slab_count, 1, LANES),
        ),
        in_specs=[VMEM, VMEM, SMEM, VMEM],
        out_specs=(VMEM,) * 4,
        scratch_shapes=rows_scratch(M_ROWS + W_ROWS, LANES),
        name="prepare",
    )(mean_flow, wall_mask, position.astype(jnp.int32).reshape(1), *held(token))
    mean_start, jacobian_x, jacobian_y = lax.optimization_barrier(
        (mean_start, jacobian_x, jacobian_y)
    )
    radial = 2 * position + jnp.arange(LANES) % 2
    radius = (HUB_RADIUS + (radial.astype(jnp.float32) + 0.5) / NZ).reshape(1, LANES)
    jac = jnp.concatenate([jacobian_x.reshape(-1, 1), jacobian_y.reshape(-1, 1)])
    jac = jnp.broadcast_to(jac, (2 * VARS * VARS, LANES))

    start, omega, speed = pl.pallas_call(
        unpack_kernel,
        out_shape=(kept(H_ROWS + 8, LANES), kept(8, LANES), kept(slab_count, 1, LANES)),
        in_specs=[VMEM] * 3,
        out_specs=(VMEM,) * 3,
        scratch_shapes=rows_scratch(LANES, 384),
        name="unpack",
    )(*held(arrived, packed, speed))

    speeds = lax.all_to_all(speed, "slab", 0, 0, tiled=True)
    cell_count = CELLS * slab_count * plane_count

    def beside(state):
        left = lax.ppermute(state, "slab", [(i, i + 1) for i in range(slab_count - 1)])
        right = lax.ppermute(state, "slab", [(i + 1, i) for i in range(slab_count - 1)])
        return state, left, right

    def section(stage, *operands):
        if stage == len(SECTION_RATES) - 1:
            shapes, scratch = kept(32, 4, 512), rows_scratch(512, LANES)
            specs = VMEM
        else:
            shapes, scratch = (kept(H_ROWS + 8, LANES), kept(M_ROWS, LANES)), []
            specs = (VMEM, VMEM)
        return pl.pallas_call(
            functools.partial(section_kernel, stage=stage, cell_count=cell_count),
            out_shape=shapes,
            in_specs=[VMEM] * len(operands),
            out_specs=specs,
            scratch_shapes=scratch,
        )(*held(*operands))

    fixed = (omega, wall, jac, radius)
    start_blocks = beside(start)
    residual, mean_residual = section(0, *start_blocks, mean_start, *fixed)
    state, mean_now = section(
        1, *start_blocks, mean_start, *fixed, speeds, *beside(residual), mean_residual
    )
    state, mean_now = section(2, *beside(state), mean_now, *fixed, speeds, start, mean_start)
    result = section(3, *beside(state), mean_now, *fixed, speeds, start, mean_start)
    back = lax.all_to_all(result, "harm", 0, 0, tiled=True)
    return pl.pallas_call(
        restore_kernel,
        out_shape=(f32(*mean_flow.shape), f32(*harmonics.shape)),
        in_specs=[VMEM],
        out_specs=(VMEM, VMEM),
        scratch_shapes=rows_scratch(LANES, 512),
        name="restore",
    )(*held(back))


def solution(mesh):
    placed = (
        P("harm", None, None, "slab", None),
        P(None, "slab", None),
        P("harm"),
        P("slab", None),
        P(),
        P(),
    )
    return jax.shard_map(
        shards,
        mesh=mesh,
        in_specs=placed,
        out_specs=(P(None, "slab", None), P("harm", None, None, "slab", None)),
        check_vma=False,
    )
```

```python
import functools

import jax
import jax.numpy as jnp
from jax import lax
from jax.experimental import pallas as pl
from jax.experimental.pallas import tpu as pltpu
from jax.sharding import PartitionSpec as P


NZ = 64
EPS_FOURTH = 0.05
COURANT = 0.9
OMEGA_BASE = 0.25
WALL_RATE = 2.0
HUB_RADIUS = 0.5
SECTION_RATES = (0.25, 1.0 / 3.0, 0.5, 1.0)
STRESS_PAIRS = ((1, 1), (1, 2), (1, 3), (2, 2), (2, 3), (3, 3), (4, 1), (4, 2), (4, 3))

VARS = 5
CELLS = 2
C1 = 16
LANES = 128
H_ROWS = 2 * VARS * CELLS * C1
M_ROWS = VARS * CELLS * C1
W_ROWS = CELLS * C1


def h_row(part, var, cell):
    return ((part * VARS + var) * CELLS + cell) * C1


def m_row(var, cell):
    return (var * CELLS + cell) * C1


def pack_kernel(harm_ref, freq_ref, out_ref, token_ref, rows_ref):
    for part in range(2):
        for var in range(VARS):
            for cell in range(CELLS):
                for c1 in range(C1):
                    row = h_row(part, var, cell) + c1
                    rows_ref[row : row + 1, :] = harm_ref[
                        0, part, var, cell : cell + 1, c1 * LANES : (c1 + 1) * LANES
                    ]
    omega = OMEGA_BASE * freq_ref[0].astype(jnp.float32)
    rows_ref[H_ROWS:, :] = jnp.full((rows_ref.shape[0] - H_ROWS, LANES), omega, jnp.float32)
    token_ref[...] = jnp.full((8, LANES), omega, jnp.float32)
    turned = rows_ref[...].T
    for j in range(32):
        out_ref[j, 0:2, :] = turned[2 * j : 2 * j + 2, :]
        out_ref[j, 2:4, :] = turned[NZ + 2 * j : NZ + 2 * j + 2, :]


def pack_mean(tiles):
    group = lax.broadcasted_iota(jnp.int32, (8, LANES), 1) // 4
    packed = jnp.zeros((8, LANES), jnp.float32)
    for i, tile in enumerate(tiles):
        for half in range(2):
            packed = jnp.where(group == 2 * i + half, tile[8 * half : 8 * half + 8, :], packed)
    return packed


def unpack_mean(packed):
    lane = lax.broadcasted_iota(jnp.int32, (8, LANES), 1) % 4
    tiles = []
    for i in range(VARS * CELLS):
        halves = [
            jnp.take_along_axis(packed, lane + 4 * (2 * i + half), axis=1) for half in range(2)
        ]
        tiles.append(jnp.concatenate(halves, axis=0))
    return tiles


def prepare_kernel(
    mean_ref, wall_ref, position_ref, token_ref, mean_out, wall_out, packed_out, speed_out, rows_ref
):
    del token_ref
    for cell in range(CELLS):
        for c1 in range(C1):
            cols = slice(c1 * LANES, (c1 + 1) * LANES)
            for var in range(VARS):
                row = m_row(var, cell) + c1
                rows_ref[row : row + 1, :] = mean_ref[var, cell : cell + 1, cols]
            row = M_ROWS + cell * C1 + c1
            rows_ref[row : row + 1, :] = wall_ref[cell : cell + 1, cols].astype(jnp.float32)
    lane = lax.broadcasted_iota(jnp.int32, (8, LANES), 1)
    source = ((lane // 2) % 2) * NZ + 2 * position_ref[0] + lane % 2
    for start in range(0, M_ROWS + W_ROWS, 8):
        picked = jnp.take_along_axis(rows_ref[start : start + 8, :], source, axis=1)
        if start < M_ROWS:
            mean_out[start : start + 8, :] = picked
        else:
            wall_out[start - M_ROWS : start - M_ROWS + 8, :] = picked
    momentum = rows_ref[m_row(1, 0) : m_row(2, 0), :]
    speed_out[...] = jnp.full(speed_out.shape, jnp.sum(momentum * momentum), jnp.float32)
    packed_out[...] = pack_mean(
        [mean_out[i * C1 : (i + 1) * C1, :] for i in range(VARS * CELLS)]
    )


def unpack_kernel(arrived_ref, packed_ref, speed_ref, state_out, omega_out, speed_out, rows_ref):
    speed_out[...] = speed_ref[...]
    for k in range(32):
        rows_ref[4 * k : 4 * k + 4, :] = arrived_ref[k]
    turned = rows_ref[...].T
    state_out[:H_ROWS, :] = turned[:H_ROWS, :]
    state_out[H_ROWS:, :] = packed_ref[...]
    omega_out[...] = turned[H_ROWS : H_ROWS + 8, :]


def section_kernel(*refs, stage, cell_count):
    last = stage == len(SECTION_RATES) - 1
    parity_ref, own_ref, core_ref, chip_ref, *refs = refs
    mean_ref, omega_ref, wall_ref, jac_ref, radius_ref, *refs = refs
    if stage == 0:
        outs = refs
    elif stage == 1:
        speed_ref, own_res, core_res, chip_res, mean_res, *outs = refs
        h0_ref, m0_ref = own_ref, mean_ref
    else:
        speed_ref, h0_ref, m0_ref, *outs = refs
    lane = lax.broadcasted_iota(jnp.int32, (C1, LANES), 1)
    even = (lane // 2) % 2 == 0

    def up(tile):
        return pltpu.roll(tile, C1 - 1, 0)

    def down(tile):
        return pltpu.roll(tile, 1, 0)

    def beside(tile):
        swapped = jnp.where(even, pltpu.roll(tile, LANES - 2, 1), pltpu.roll(tile, 2, 1))
        return jnp.where(even, swapped, up(swapped)), jnp.where(even, down(swapped), swapped)

    def splat(ref, row):
        return jnp.broadcast_to(ref[row : row + 1, :], (C1, LANES))

    def apply_matrix(base, tiles):
        out = []
        for a in range(VARS):
            total = splat(jac_ref, base + VARS * a) * tiles[0]
            for b in range(1, VARS):
                total = total + splat(jac_ref, base + VARS * a + b) * tiles[b]
            out.append(total)
        return out

    omega = splat(omega_ref, 0)
    if stage:
        speed_total = jnp.sum(speed_ref[...], axis=0)
        time_step = COURANT / (1.0 + jnp.sqrt(speed_total / cell_count))
        time_step = jnp.broadcast_to(time_step, (C1, LANES))
        step = SECTION_RATES[stage] * time_step
    own, core, chip = (own_ref, None), (core_ref, None), (chip_ref, None)
    mean_block = (mean_ref, None)
    if stage == 1:
        first = SECTION_RATES[0] * time_step
        own, core, chip = (own_ref, own_res), (core_ref, core_res), (chip_ref, chip_res)
        mean_block = (mean_ref, mean_res)

    def load(block, row, count=C1):
        base, residual = block
        value = base[row : row + count, :]
        if residual is not None:
            value = value + first[:count] * residual[row : row + count, :]
        return value

    on_first = parity_ref[0] == 0

    def sides(row, count=C1):
        paired, other = load(core, row, count), load(chip, row, count)
        return jnp.where(on_first, other, paired), jnp.where(on_first, paired, other)

    def column(part, var):
        rows = [h_row(part, var, cell) for cell in range(CELLS)]
        left, right = zip(*[sides(row) for row in rows])
        return [*left, *[load(own, row) for row in rows], *right]

    inv_radius = 1.0 / splat(radius_ref, 0)

    harm = [[column(part, var) for var in range(VARS)] for part in range(2)]
    left_mean, right_mean = [unpack_mean(packed) for packed in sides(H_ROWS, 8)]
    mean = []
    for var in range(VARS):
        own_mean = [load(mean_block, m_row(var, cell)) for cell in range(CELLS)]
        mean.append(
            left_mean[CELLS * var : CELLS * (var + 1)]
            + own_mean
            + right_mean[CELLS * var : CELLS * (var + 1)]
        )

    def smooth_parts(cells, at):
        center = cells[at]
        above, below = beside(center)
        diff_y = (above - below) * 0.5
        fourth = (
            (cells[at + 2] + cells[at - 2])
            + (up(center) + down(center))
            - 4.0 * ((cells[at + 1] + cells[at - 1]) + (above + below))
            + 12.0 * center
        )
        return diff_y, fourth

    harm_new = {}
    for cell in range(CELLS):
        at = 2 + cell
        wall = WALL_RATE * wall_ref[cell * C1 : (cell + 1) * C1, :]
        for part in range(2):
            diffs_x, diffs_y, fourths = [], [], []
            for var in range(VARS):
                cells = harm[part][var]
                diffs_x.append(
                    (mean[1][at + 1] * cells[at + 1] - mean[1][at - 1] * cells[at - 1]) * 0.5
                )
                diff_y, fourth = smooth_parts(cells, at)
                diffs_y.append(diff_y)
                fourths.append(fourth)
            flux_x = apply_matrix(0, diffs_x)
            flux_y = apply_matrix(VARS * VARS, diffs_y)
            for var in range(VARS):
                turned = omega * harm[1 - part][var][at]
                if part:
                    turned = -turned
                res = (
                    turned
                    - flux_x[var]
                    - flux_y[var]
                    - EPS_FOURTH * fourths[var]
                    - wall * harm[part][var][at]
                )
                row = h_row(part, var, cell)
                if stage:
                    res = h0_ref[row : row + C1, :] + step * res
                harm_new[part, var, cell] = res

    def stress(index, at):
        a, b = STRESS_PAIRS[index]
        return 0.5 * (harm[0][a][at] * harm[0][b][at] + harm[1][a][at] * harm[1][b][at])

    def total(tile):
        for shift in (4, 8, 16, 32, 64):
            tile = tile + pltpu.roll(tile, shift, 1)
        return jnp.take_along_axis(tile, lane % 4, axis=1)

    mean_new = {}
    for cell in range(CELLS):
        at = 2 + cell

        def grad_x(index):
            return (stress(index, at + 1) - stress(index, at - 1)) * 0.5

        def grad_y(tile):
            above, below = beside(tile)
            return (above - below) * 0.5

        s3, s4 = stress(3, at), stress(4, at)
        terms = [
            None,
            total(-grad_x(0) - grad_y(stress(1, at))),
            total(-grad_x(1) - grad_y(s3) - 2.0 * s4 * inv_radius),
            total(-grad_x(2) - grad_y(s4) + (s3 - stress(5, at)) * inv_radius),
            total(-grad_x(6) - grad_y(stress(7, at)) - stress(8, at) * inv_radius),
        ]
        diffs_x, diffs_y, fourths = [], [], []
        for var in range(VARS):
            cells = mean[var]
            diffs_x.append((cells[at + 1] - cells[at - 1]) * 0.5)
            diff_y, fourth = smooth_parts(cells, at)
            diffs_y.append(diff_y)
            fourths.append(fourth)
        flux_x = apply_matrix(0, diffs_x)
        flux_y = apply_matrix(VARS * VARS, diffs_y)
        for var in range(VARS):
            res = -flux_x[var] - flux_y[var] - EPS_FOURTH * fourths[var]
            if var:
                res = res + terms[var]
            row = m_row(var, cell)
            if stage:
                res = m0_ref[row : row + C1, :] + step * res
            mean_new[var, cell] = res

    if last:
        out_ref, rows_ref = outs
        target, offset = rows_ref, H_ROWS
    else:
        state_out, mean_out = outs
        target, offset = state_out, None
    for (part, var, cell), tile in harm_new.items():
        row = h_row(part, var, cell)
        target[row : row + C1, :] = tile
    for (var, cell), tile in mean_new.items():
        row = m_row(var, cell)
        if last:
            target[offset + row : offset + row + C1, :] = tile
        else:
            mean_out[row : row + C1, :] = tile
    if last:
        spare = H_ROWS + M_ROWS
        rows_ref[spare:, :] = jnp.zeros((rows_ref.shape[0] - spare, LANES), jnp.float32)
        turned = rows_ref[...].T
        for k in range(32):
            out_ref[k] = turned[4 * k : 4 * k + 4, :]
    else:
        state_out[H_ROWS:, :] = pack_mean(
            [mean_new[var, cell] for var in range(VARS) for cell in range(CELLS)]
        )


def restore_kernel(arrived_ref, mean_out, harm_out, rows_ref):
    for j in range(32):
        rows_ref[2 * j : 2 * j + 2, :] = arrived_ref[j, 0:2, :]
        rows_ref[NZ + 2 * j : NZ + 2 * j + 2, :] = arrived_ref[j, 2:4, :]
    turned = rows_ref[...].T
    for var in range(VARS):
        for cell in range(CELLS):
            for c1 in range(C1):
                cols = slice(c1 * LANES, (c1 + 1) * LANES)
                for part in range(2):
                    row = h_row(part, var, cell) + c1
                    harm_out[0, part, var, cell : cell + 1, cols] = turned[row : row + 1, :]
                row = H_ROWS + m_row(var, cell) + c1
                mean_out[var, cell : cell + 1, cols] = turned[row : row + 1, :]


def f32(*shape):
    return jax.ShapeDtypeStruct(shape, jnp.float32)


def kept(*shape):
    return pltpu.VMEM(shape, jnp.float32)


def held(*arrays):
    return [pltpu.with_memory_space_constraint(array, pltpu.VMEM) for array in arrays]


VMEM = pl.BlockSpec(memory_space=pltpu.VMEM)
SMEM = pl.BlockSpec(memory_space=pltpu.SMEM)


def rows_scratch(*shape):
    return [pltpu.VMEM(shape, jnp.float32)]


def shards(harmonics, mean_flow, freq_index, wall_mask, jacobian_x, jacobian_y):
    plane_count = mean_flow.shape[2]
    slab_count = lax.axis_size("slab")
    position = lax.axis_index("harm")

    sends, token = pl.pallas_call(
        pack_kernel,
        out_shape=(kept(32, 4, 384), kept(8, LANES)),
        in_specs=[VMEM, SMEM],
        out_specs=(VMEM, VMEM),
        scratch_shapes=rows_scratch(384, LANES),
        name="pack",
    )(harmonics, freq_index)
    arrived = lax.all_to_all(sends, "harm", 0, 0, tiled=True)

    mean_start, wall, packed, speed = pl.pallas_call(
        prepare_kernel,
        out_shape=(
            kept(M_ROWS, LANES),
            kept(W_ROWS, LANES),
            kept(8, LANES),
            kept(slab_count, 1, LANES),
        ),
        in_specs=[VMEM, VMEM, SMEM, VMEM],
        out_specs=(VMEM,) * 4,
        scratch_shapes=rows_scratch(M_ROWS + W_ROWS, LANES),
        name="prepare",
    )(mean_flow, wall_mask, position.astype(jnp.int32).reshape(1), *held(token))
    mean_start, jacobian_x, jacobian_y = lax.optimization_barrier(
        (mean_start, jacobian_x, jacobian_y)
    )
    radial = 2 * position + jnp.arange(LANES) % 2
    radius = (HUB_RADIUS + (radial.astype(jnp.float32) + 0.5) / NZ).reshape(1, LANES)
    jac = jnp.concatenate([jacobian_x.reshape(-1, 1), jacobian_y.reshape(-1, 1)])
    jac = jnp.broadcast_to(jac, (2 * VARS * VARS, LANES))

    start, omega, speed = pl.pallas_call(
        unpack_kernel,
        out_shape=(kept(H_ROWS + 8, LANES), kept(8, LANES), kept(slab_count, 1, LANES)),
        in_specs=[VMEM] * 3,
        out_specs=(VMEM,) * 3,
        scratch_shapes=rows_scratch(LANES, 384),
        name="unpack",
    )(*held(arrived, packed, speed))

    speeds = lax.all_to_all(speed, "slab", 0, 0, tiled=True)
    cell_count = CELLS * slab_count * plane_count

    core_pairs = [(i, i ^ 1) for i in range(slab_count)]
    chip_pairs = [
        pair for i in range(1, slab_count - 1, 2) for pair in ((i, i + 1), (i + 1, i))
    ]

    def beside(state):
        core = lax.ppermute(state, "slab", core_pairs)
        chip = lax.ppermute(state, "slab", chip_pairs)
        return state, core, chip

    def section(stage, *operands):
        if stage == len(SECTION_RATES) - 1:
            shapes, scratch = kept(32, 4, 512), rows_scratch(512, LANES)
            specs = VMEM
        else:
            shapes, scratch = (kept(H_ROWS + 8, LANES), kept(M_ROWS, LANES)), []
            specs = (VMEM, VMEM)
        return pl.pallas_call(
            functools.partial(section_kernel, stage=stage, cell_count=cell_count),
            out_shape=shapes,
            in_specs=[SMEM] + [VMEM] * len(operands),
            out_specs=specs,
            scratch_shapes=scratch,
        )(parity, *held(*operands))

    parity = (lax.axis_index("slab") % 2).astype(jnp.int32).reshape(1)
    fixed = (omega, wall, jac, radius)
    start_blocks = beside(start)
    residual, mean_residual = section(0, *start_blocks, mean_start, *fixed)
    state, mean_now = section(
        1, *start_blocks, mean_start, *fixed, speeds, *beside(residual), mean_residual
    )
    state, mean_now = section(2, *beside(state), mean_now, *fixed, speeds, start, mean_start)
    result = section(3, *beside(state), mean_now, *fixed, speeds, start, mean_start)
    back = lax.all_to_all(result, "harm", 0, 0, tiled=True)
    return pl.pallas_call(
        restore_kernel,
        out_shape=(f32(*mean_flow.shape), f32(*harmonics.shape)),
        in_specs=[VMEM],
        out_specs=(VMEM, VMEM),
        scratch_shapes=rows_scratch(LANES, 512),
        name="restore",
    )(*held(back))


def solution(mesh):
    placed = (
        P("harm", None, None, "slab", None),
        P(None, "slab", None),
        P("harm"),
        P("slab", None),
        P(),
        P(),
    )
    return jax.shard_map(
        shards,
        mesh=mesh,
        in_specs=placed,
        out_specs=(P(None, "slab", None), P("harm", None, None, "slab", None)),
        check_vma=False,
    )
```

```python
import functools

import jax
import jax.numpy as jnp
from jax import lax
from jax.experimental import pallas as pl
from jax.experimental.pallas import tpu as pltpu
from jax.sharding import PartitionSpec as P


NZ = 64
EPS_FOURTH = 0.05
COURANT = 0.9
OMEGA_BASE = 0.25
WALL_RATE = 2.0
HUB_RADIUS = 0.5
SECTION_RATES = (0.25, 1.0 / 3.0, 0.5, 1.0)
STRESS_PAIRS = ((1, 1), (1, 2), (1, 3), (2, 2), (2, 3), (3, 3), (4, 1), (4, 2), (4, 3))

VARS = 5
CELLS = 2
C1 = 16
LANES = 128
H_ROWS = 2 * VARS * CELLS * C1
M_ROWS = VARS * CELLS * C1
W_ROWS = CELLS * C1


def h_row(part, var, cell):
    return ((part * VARS + var) * CELLS + cell) * C1


def m_row(var, cell):
    return (var * CELLS + cell) * C1


def pack_kernel(harm_ref, freq_ref, out_ref, token_ref, rows_ref):
    for part in range(2):
        for var in range(VARS):
            for cell in range(CELLS):
                for c1 in range(C1):
                    row = h_row(part, var, cell) + c1
                    rows_ref[row : row + 1, :] = harm_ref[
                        0, part, var, cell : cell + 1, c1 * LANES : (c1 + 1) * LANES
                    ]
    omega = OMEGA_BASE * freq_ref[0].astype(jnp.float32)
    rows_ref[H_ROWS:, :] = jnp.full((rows_ref.shape[0] - H_ROWS, LANES), omega, jnp.float32)
    token_ref[...] = jnp.full((8, LANES), omega, jnp.float32)
    turned = rows_ref[...].T
    for j in range(32):
        out_ref[j, 0:2, :] = turned[2 * j : 2 * j + 2, :]
        out_ref[j, 2:4, :] = turned[NZ + 2 * j : NZ + 2 * j + 2, :]


def pack_mean(tiles):
    group = lax.broadcasted_iota(jnp.int32, (8, LANES), 1) // 4
    packed = jnp.zeros((8, LANES), jnp.float32)
    for i, tile in enumerate(tiles):
        for half in range(2):
            packed = jnp.where(group == 2 * i + half, tile[8 * half : 8 * half + 8, :], packed)
    return packed


def unpack_mean(packed):
    lane = lax.broadcasted_iota(jnp.int32, (8, LANES), 1) % 4
    tiles = []
    for i in range(VARS * CELLS):
        halves = [
            jnp.take_along_axis(packed, lane + 4 * (2 * i + half), axis=1) for half in range(2)
        ]
        tiles.append(jnp.concatenate(halves, axis=0))
    return tiles


def prepare_kernel(
    mean_ref, wall_ref, jac_x_ref, jac_y_ref, position_ref, token_ref,
    mean_out, wall_out, packed_out, speed_out, jac_out, rows_ref
):
    del token_ref
    for base, matrix_ref in ((0, jac_x_ref), (VARS * VARS, jac_y_ref)):
        for a in range(VARS):
            for b in range(VARS):
                row = base + VARS * a + b
                jac_out[row : row + 1, :] = jnp.broadcast_to(
                    matrix_ref[a : a + 1, b : b + 1], (1, LANES)
                )
    for cell in range(CELLS):
        for c1 in range(C1):
            cols = slice(c1 * LANES, (c1 + 1) * LANES)
            for var in range(VARS):
                row = m_row(var, cell) + c1
                rows_ref[row : row + 1, :] = mean_ref[var, cell : cell + 1, cols]
            row = M_ROWS + cell * C1 + c1
            rows_ref[row : row + 1, :] = wall_ref[cell : cell + 1, cols].astype(jnp.float32)
    lane = lax.broadcasted_iota(jnp.int32, (8, LANES), 1)
    source = ((lane // 2) % 2) * NZ + 2 * position_ref[0] + lane % 2
    for start in range(0, M_ROWS + W_ROWS, 8):
        picked = jnp.take_along_axis(rows_ref[start : start + 8, :], source, axis=1)
        if start < M_ROWS:
            mean_out[start : start + 8, :] = picked
        else:
            wall_out[start - M_ROWS : start - M_ROWS + 8, :] = picked
    momentum = rows_ref[m_row(1, 0) : m_row(2, 0), :]
    speed_out[...] = jnp.full(speed_out.shape, jnp.sum(momentum * momentum), jnp.float32)
    packed_out[...] = pack_mean(
        [mean_out[i * C1 : (i + 1) * C1, :] for i in range(VARS * CELLS)]
    )


def unpack_kernel(arrived_ref, packed_ref, speed_ref, state_out, omega_out, rows_ref):
    del speed_ref
    for k in range(32):
        rows_ref[4 * k : 4 * k + 4, :] = arrived_ref[k]
    turned = rows_ref[...].T
    state_out[:H_ROWS, :] = turned[:H_ROWS, :]
    state_out[H_ROWS:, :] = packed_ref[...]
    omega_out[...] = turned[H_ROWS : H_ROWS + 8, :]


def section_kernel(*refs, stage, cell_count):
    last = stage == len(SECTION_RATES) - 1
    parity_ref, own_ref, core_ref, chip_ref, *refs = refs
    mean_ref, omega_ref, wall_ref, jac_ref, radius_ref, *refs = refs
    if stage < 2:
        speed_ref, beside_ref, *refs = refs
        speed = speed_ref[...] + beside_ref[...]
    if stage == 0:
        *outs, speed_out = refs
        speed_out[...] = speed
    elif stage == 1:
        own_res, core_res, chip_res, mean_res, *outs, step_out = refs
        h0_ref, m0_ref = own_ref, mean_ref
        time_step = COURANT / (1.0 + jnp.sqrt(speed / cell_count))
        step_out[...] = time_step
    else:
        step_ref, h0_ref, m0_ref, *outs = refs
        time_step = step_ref[...]
    if stage:
        time_step = jnp.concatenate([time_step, time_step], axis=0)

    lane = lax.broadcasted_iota(jnp.int32, (C1, LANES), 1)
    even = (lane // 2) % 2 == 0

    def up(tile):
        return pltpu.roll(tile, C1 - 1, 0)

    def down(tile):
        return pltpu.roll(tile, 1, 0)

    def beside(tile):
        swapped = jnp.where(even, pltpu.roll(tile, LANES - 2, 1), pltpu.roll(tile, 2, 1))
        return jnp.where(even, swapped, up(swapped)), jnp.where(even, down(swapped), swapped)

    def splat(ref, row):
        return jnp.broadcast_to(ref[row : row + 1, :], (C1, LANES))

    def apply_matrix(base, tiles):
        out = []
        for a in range(VARS):
            total = splat(jac_ref, base + VARS * a) * tiles[0]
            for b in range(1, VARS):
                total = total + splat(jac_ref, base + VARS * a + b) * tiles[b]
            out.append(total)
        return out

    omega = splat(omega_ref, 0)
    if stage:
        step = SECTION_RATES[stage] * time_step
    own, core, chip = (own_ref, None), (core_ref, None), (chip_ref, None)
    mean_block = (mean_ref, None)
    if stage == 1:
        first = SECTION_RATES[0] * time_step
        own, core, chip = (own_ref, own_res), (core_ref, core_res), (chip_ref, chip_res)
        mean_block = (mean_ref, mean_res)

    def load(block, row, count=C1):
        base, residual = block
        value = base[row : row + count, :]
        if residual is not None:
            value = value + first[:count] * residual[row : row + count, :]
        return value

    on_first = parity_ref[0] == 0

    def sides(row, count=C1):
        paired, other = load(core, row, count), load(chip, row, count)
        return jnp.where(on_first, other, paired), jnp.where(on_first, paired, other)

    def column(part, var):
        rows = [h_row(part, var, cell) for cell in range(CELLS)]
        left, right = zip(*[sides(row) for row in rows])
        return [*left, *[load(own, row) for row in rows], *right]

    inv_radius = 1.0 / splat(radius_ref, 0)

    harm = [[column(part, var) for var in range(VARS)] for part in range(2)]
    left_mean, right_mean = [unpack_mean(packed) for packed in sides(H_ROWS, 8)]
    mean = []
    for var in range(VARS):
        own_mean = [load(mean_block, m_row(var, cell)) for cell in range(CELLS)]
        mean.append(
            left_mean[CELLS * var : CELLS * (var + 1)]
            + own_mean
            + right_mean[CELLS * var : CELLS * (var + 1)]
        )

    def smooth_parts(cells, at):
        center = cells[at]
        above, below = beside(center)
        diff_y = (above - below) * 0.5
        fourth = (
            (cells[at + 2] + cells[at - 2])
            + (up(center) + down(center))
            - 4.0 * ((cells[at + 1] + cells[at - 1]) + (above + below))
            + 12.0 * center
        )
        return diff_y, fourth

    harm_new = {}
    for cell in range(CELLS):
        at = 2 + cell
        wall = WALL_RATE * wall_ref[cell * C1 : (cell + 1) * C1, :]
        for part in range(2):
            diffs_x, diffs_y, fourths = [], [], []
            for var in range(VARS):
                cells = harm[part][var]
                diffs_x.append(
                    (mean[1][at + 1] * cells[at + 1] - mean[1][at - 1] * cells[at - 1]) * 0.5
                )
                diff_y, fourth = smooth_parts(cells, at)
                diffs_y.append(diff_y)
                fourths.append(fourth)
            flux_x = apply_matrix(0, diffs_x)
            flux_y = apply_matrix(VARS * VARS, diffs_y)
            for var in range(VARS):
                turned = omega * harm[1 - part][var][at]
                if part:
                    turned = -turned
                res = (
                    turned
                    - flux_x[var]
                    - flux_y[var]
                    - EPS_FOURTH * fourths[var]
                    - wall * harm[part][var][at]
                )
                row = h_row(part, var, cell)
                if stage:
                    res = h0_ref[row : row + C1, :] + step * res
                harm_new[part, var, cell] = res

    def stress(index, at):
        a, b = STRESS_PAIRS[index]
        return 0.5 * (harm[0][a][at] * harm[0][b][at] + harm[1][a][at] * harm[1][b][at])

    def total(tile):
        for shift in (4, 8, 16, 32, 64):
            tile = tile + pltpu.roll(tile, shift, 1)
        return jnp.take_along_axis(tile, lane % 4, axis=1)

    mean_new = {}
    for cell in range(CELLS):
        at = 2 + cell

        def grad_x(index):
            return (stress(index, at + 1) - stress(index, at - 1)) * 0.5

        def grad_y(tile):
            above, below = beside(tile)
            return (above - below) * 0.5

        s3, s4 = stress(3, at), stress(4, at)
        terms = [
            None,
            total(-grad_x(0) - grad_y(stress(1, at))),
            total(-grad_x(1) - grad_y(s3) - 2.0 * s4 * inv_radius),
            total(-grad_x(2) - grad_y(s4) + (s3 - stress(5, at)) * inv_radius),
            total(-grad_x(6) - grad_y(stress(7, at)) - stress(8, at) * inv_radius),
        ]
        diffs_x, diffs_y, fourths = [], [], []
        for var in range(VARS):
            cells = mean[var]
            diffs_x.append((cells[at + 1] - cells[at - 1]) * 0.5)
            diff_y, fourth = smooth_parts(cells, at)
            diffs_y.append(diff_y)
            fourths.append(fourth)
        flux_x = apply_matrix(0, diffs_x)
        flux_y = apply_matrix(VARS * VARS, diffs_y)
        for var in range(VARS):
            res = -flux_x[var] - flux_y[var] - EPS_FOURTH * fourths[var]
            if var:
                res = res + terms[var]
            row = m_row(var, cell)
            if stage:
                res = m0_ref[row : row + C1, :] + step * res
            mean_new[var, cell] = res

    if last:
        out_ref, rows_ref = outs
        target, offset = rows_ref, H_ROWS
    else:
        state_out, mean_out = outs
        target, offset = state_out, None
    for (part, var, cell), tile in harm_new.items():
        row = h_row(part, var, cell)
        target[row : row + C1, :] = tile
    for (var, cell), tile in mean_new.items():
        row = m_row(var, cell)
        if last:
            target[offset + row : offset + row + C1, :] = tile
        else:
            mean_out[row : row + C1, :] = tile
    if last:
        spare = H_ROWS + M_ROWS
        rows_ref[spare:, :] = jnp.zeros((rows_ref.shape[0] - spare, LANES), jnp.float32)
        turned = rows_ref[...].T
        for k in range(32):
            out_ref[k] = turned[4 * k : 4 * k + 4, :]
    else:
        state_out[H_ROWS:, :] = pack_mean(
            [mean_new[var, cell] for var in range(VARS) for cell in range(CELLS)]
        )


def restore_kernel(arrived_ref, mean_out, harm_out, rows_ref):
    for j in range(32):
        rows_ref[2 * j : 2 * j + 2, :] = arrived_ref[j, 0:2, :]
        rows_ref[NZ + 2 * j : NZ + 2 * j + 2, :] = arrived_ref[j, 2:4, :]
    turned = rows_ref[...].T
    for var in range(VARS):
        for cell in range(CELLS):
            for c1 in range(C1):
                cols = slice(c1 * LANES, (c1 + 1) * LANES)
                for part in range(2):
                    row = h_row(part, var, cell) + c1
                    harm_out[0, part, var, cell : cell + 1, cols] = turned[row : row + 1, :]
                row = H_ROWS + m_row(var, cell) + c1
                mean_out[var, cell : cell + 1, cols] = turned[row : row + 1, :]


def f32(*shape):
    return jax.ShapeDtypeStruct(shape, jnp.float32)


def kept(*shape):
    return pltpu.VMEM(shape, jnp.float32)


def held(*arrays):
    return [pltpu.with_memory_space_constraint(array, pltpu.VMEM) for array in arrays]


VMEM = pl.BlockSpec(memory_space=pltpu.VMEM)
SMEM = pl.BlockSpec(memory_space=pltpu.SMEM)


def rows_scratch(*shape):
    return [pltpu.VMEM(shape, jnp.float32)]


def shards(harmonics, mean_flow, freq_index, wall_mask, jacobian_x, jacobian_y):
    plane_count = mean_flow.shape[2]
    slab_count = lax.axis_size("slab")
    position = lax.axis_index("harm")

    sends, token = pl.pallas_call(
        pack_kernel,
        out_shape=(kept(32, 4, 384), kept(8, LANES)),
        in_specs=[VMEM, SMEM],
        out_specs=(VMEM, VMEM),
        scratch_shapes=rows_scratch(384, LANES),
        name="pack",
    )(harmonics, freq_index)
    arrived = lax.all_to_all(sends, "harm", 0, 0, tiled=True)

    mean_start, wall, packed, speed, jac = pl.pallas_call(
        prepare_kernel,
        out_shape=(
            kept(M_ROWS, LANES),
            kept(W_ROWS, LANES),
            kept(8, LANES),
            kept(8, LANES),
            kept(2 * VARS * VARS, LANES),
        ),
        in_specs=[VMEM] * 4 + [SMEM, VMEM],
        out_specs=(VMEM,) * 5,
        scratch_shapes=rows_scratch(M_ROWS + W_ROWS, LANES),
        name="prepare",
    )(
        mean_flow, wall_mask, jacobian_x, jacobian_y, position.astype(jnp.int32).reshape(1),
        *held(token)
    )

    def crossed(value, reach):
        return lax.ppermute(value, "slab", [(i, i ^ reach) for i in range(slab_count)])

    cell_count = CELLS * slab_count * plane_count
    for reach in (1, 2):
        speed = speed + crossed(speed, reach)
    radial = 2 * position + jnp.arange(LANES) % 2
    radius = (HUB_RADIUS + (radial.astype(jnp.float32) + 0.5) / NZ).reshape(1, LANES)

    start, omega = pl.pallas_call(
        unpack_kernel,
        out_shape=(kept(H_ROWS + 8, LANES), kept(8, LANES)),
        in_specs=[VMEM] * 3,
        out_specs=(VMEM,) * 2,
        scratch_shapes=rows_scratch(LANES, 384),
        name="unpack",
    )(*held(arrived, packed, speed))

    core_pairs = [(i, i ^ 1) for i in range(slab_count)]
    chip_pairs = [
        pair for i in range(1, slab_count - 1, 2) for pair in ((i, i + 1), (i + 1, i))
    ]

    def beside(state):
        core = lax.ppermute(state, "slab", core_pairs)
        chip = lax.ppermute(state, "slab", chip_pairs)
        return state, core, chip

    def section(stage, *operands):
        shapes = [kept(H_ROWS + 8, LANES), kept(M_ROWS, LANES), kept(8, LANES)]
        scratch = []
        if stage == len(SECTION_RATES) - 1:
            shapes, scratch = [kept(32, 4, 512)], rows_scratch(512, LANES)
        elif stage == len(SECTION_RATES) - 2:
            del shapes[2]
        return pl.pallas_call(
            functools.partial(section_kernel, stage=stage, cell_count=cell_count),
            out_shape=shapes,
            in_specs=[SMEM] + [VMEM] * len(operands),
            out_specs=[VMEM] * len(shapes),
            scratch_shapes=scratch,
        )(parity, *held(*operands))

    parity = (lax.axis_index("slab") % 2).astype(jnp.int32).reshape(1)
    fixed = (omega, wall, jac, radius)
    blocks = beside(start)
    speed_beside = crossed(speed, 4)
    residual, mean_residual, speed = section(0, *blocks, mean_start, *fixed, speed, speed_beside)
    residual_blocks = beside(residual)
    speed_beside = crossed(speed, 8)
    state, mean_now, step = section(
        1, *blocks, mean_start, *fixed, speed, speed_beside, *residual_blocks, mean_residual
    )
    state, mean_now = section(2, *beside(state), mean_now, *fixed, step, start, mean_start)
    (result,) = section(3, *beside(state), mean_now, *fixed, step, start, mean_start)
    back = lax.all_to_all(result, "harm", 0, 0, tiled=True)
    return pl.pallas_call(
        restore_kernel,
        out_shape=(f32(*mean_flow.shape), f32(*harmonics.shape)),
        in_specs=[VMEM],
        out_specs=(VMEM, VMEM),
        scratch_shapes=rows_scratch(LANES, 512),
        name="restore",
    )(*held(back))


def solution(mesh):
    placed = (
        P("harm", None, None, "slab", None),
        P(None, "slab", None),
        P("harm"),
        P("slab", None),
        P(),
        P(),
    )
    return jax.shard_map(
        shards,
        mesh=mesh,
        in_specs=placed,
        out_specs=(P(None, "slab", None), P("harm", None, None, "slab", None)),
        check_vma=False,
    )
```

```python
import functools

import jax
import jax.numpy as jnp
from jax import lax
from jax.experimental import pallas as pl
from jax.experimental.pallas import tpu as pltpu
from jax.sharding import PartitionSpec as P


NZ = 64
EPS_FOURTH = 0.05
COURANT = 0.9
OMEGA_BASE = 0.25
WALL_RATE = 2.0
HUB_RADIUS = 0.5
SECTION_RATES = (0.25, 1.0 / 3.0, 0.5, 1.0)
STRESS_PAIRS = ((1, 1), (1, 2), (1, 3), (2, 2), (2, 3), (3, 3), (4, 1), (4, 2), (4, 3))

VARS = 5
CELLS = 2
C1 = 16
LANES = 128
H_ROWS = 2 * VARS * CELLS * C1
M_ROWS = VARS * CELLS * C1
W_ROWS = CELLS * C1


def h_row(part, var, cell):
    return ((part * VARS + var) * CELLS + cell) * C1


def m_row(var, cell):
    return (var * CELLS + cell) * C1


def pack_mean(tiles):
    group = lax.broadcasted_iota(jnp.int32, (8, LANES), 1) // 4
    packed = jnp.zeros((8, LANES), jnp.float32)
    for i, tile in enumerate(tiles):
        for half in range(2):
            packed = jnp.where(group == 2 * i + half, tile[8 * half : 8 * half + 8, :], packed)
    return packed


def unpack_mean(packed):
    lane = lax.broadcasted_iota(jnp.int32, (8, LANES), 1) % 4
    tiles = []
    for i in range(VARS * CELLS):
        halves = [
            jnp.take_along_axis(packed, lane + 4 * (2 * i + half), axis=1) for half in range(2)
        ]
        tiles.append(jnp.concatenate(halves, axis=0))
    return tiles


def open_kernel(
    harm_ref, mean_ref, wall_ref, jac_x_ref, jac_y_ref, freq_ref, position_ref,
    out_ref, mean_out, wall_out, packed_out, speed_out, jac_out, radius_out,
    rows_ref, plane_ref
):
    for cell in range(CELLS):
        for c1 in range(C1):
            cols = slice(c1 * LANES, (c1 + 1) * LANES)
            for var in range(VARS):
                for part in range(2):
                    row = h_row(part, var, cell) + c1
                    rows_ref[row : row + 1, :] = harm_ref[0, part, var, cell : cell + 1, cols]
                row = m_row(var, cell) + c1
                plane_ref[row : row + 1, :] = mean_ref[var, cell : cell + 1, cols]
            row = M_ROWS + cell * C1 + c1
            plane_ref[row : row + 1, :] = wall_ref[cell : cell + 1, cols].astype(jnp.float32)
    omega = OMEGA_BASE * freq_ref[0].astype(jnp.float32)
    rows_ref[H_ROWS:, :] = jnp.full((rows_ref.shape[0] - H_ROWS, LANES), omega, jnp.float32)
    turned = rows_ref[...].T
    for j in range(32):
        out_ref[j, 0:2, :] = turned[2 * j : 2 * j + 2, :]
        out_ref[j, 2:4, :] = turned[NZ + 2 * j : NZ + 2 * j + 2, :]

    for base, matrix_ref in ((0, jac_x_ref), (VARS * VARS, jac_y_ref)):
        for a in range(VARS):
            for b in range(VARS):
                row = base + VARS * a + b
                jac_out[row : row + 1, :] = jnp.broadcast_to(
                    matrix_ref[a : a + 1, b : b + 1], (1, LANES)
                )
    lane = lax.broadcasted_iota(jnp.int32, (8, LANES), 1)
    radial = 2 * position_ref[0] + lane % 2
    radius_out[...] = HUB_RADIUS + (radial.astype(jnp.float32) + 0.5) / NZ
    source = ((lane // 2) % 2) * NZ + radial
    for start in range(0, M_ROWS + W_ROWS, 8):
        picked = jnp.take_along_axis(plane_ref[start : start + 8, :], source, axis=1)
        if start < M_ROWS:
            mean_out[start : start + 8, :] = picked
        else:
            wall_out[start - M_ROWS : start - M_ROWS + 8, :] = picked
    momentum = plane_ref[m_row(1, 0) : m_row(2, 0), :]
    speed_out[...] = jnp.full(speed_out.shape, jnp.sum(momentum * momentum), jnp.float32)
    packed_out[...] = pack_mean(
        [mean_out[i * C1 : (i + 1) * C1, :] for i in range(VARS * CELLS)]
    )


def unpack_kernel(arrived_ref, packed_ref, state_out, omega_out, rows_ref):
    for k in range(32):
        rows_ref[4 * k : 4 * k + 4, :] = arrived_ref[k]
    turned = rows_ref[...].T
    state_out[:H_ROWS, :] = turned[:H_ROWS, :]
    state_out[H_ROWS:, :] = packed_ref[...]
    omega_out[...] = turned[H_ROWS : H_ROWS + 8, :]


def section_kernel(*refs, stage, cell_count):
    last = stage == len(SECTION_RATES) - 1
    parity_ref, own_ref, core_ref, chip_ref, *refs = refs
    mean_ref, omega_ref, wall_ref, jac_ref, radius_ref, *refs = refs
    if stage == 0:
        outs = refs
    elif stage == 1:
        speed_ref, own_res, core_res, chip_res, mean_res, *outs = refs
        h0_ref, m0_ref = own_ref, mean_ref
    else:
        speed_ref, h0_ref, m0_ref, *outs = refs
    lane = lax.broadcasted_iota(jnp.int32, (C1, LANES), 1)
    even = (lane // 2) % 2 == 0

    def up(tile):
        return pltpu.roll(tile, C1 - 1, 0)

    def down(tile):
        return pltpu.roll(tile, 1, 0)

    def beside(tile):
        swapped = jnp.where(even, pltpu.roll(tile, LANES - 2, 1), pltpu.roll(tile, 2, 1))
        return jnp.where(even, swapped, up(swapped)), jnp.where(even, down(swapped), swapped)

    def splat(ref, row):
        return jnp.broadcast_to(ref[row : row + 1, :], (C1, LANES))

    def apply_matrix(base, tiles):
        out = []
        for a in range(VARS):
            total = splat(jac_ref, base + VARS * a) * tiles[0]
            for b in range(1, VARS):
                total = total + splat(jac_ref, base + VARS * a + b) * tiles[b]
            out.append(total)
        return out

    omega = splat(omega_ref, 0)
    if stage:
        speed_total = jnp.sum(speed_ref[...], axis=0)
        time_step = COURANT / (1.0 + jnp.sqrt(speed_total / cell_count))
        time_step = jnp.broadcast_to(time_step, (C1, LANES))
        step = SECTION_RATES[stage] * time_step
    own, core, chip = (own_ref, None), (core_ref, None), (chip_ref, None)
    mean_block = (mean_ref, None)
    if stage == 1:
        first = SECTION_RATES[0] * time_step
        own, core, chip = (own_ref, own_res), (core_ref, core_res), (chip_ref, chip_res)
        mean_block = (mean_ref, mean_res)

    def load(block, row, count=C1):
        base, residual = block
        value = base[row : row + count, :]
        if residual is not None:
            value = value + first[:count] * residual[row : row + count, :]
        return value

    on_first = parity_ref[0] == 0

    def sides(row, count=C1):
        paired, other = load(core, row, count), load(chip, row, count)
        return jnp.where(on_first, other, paired), jnp.where(on_first, paired, other)

    def column(part, var):
        rows = [h_row(part, var, cell) for cell in range(CELLS)]
        left, right = zip(*[sides(row) for row in rows])
        return [*left, *[load(own, row) for row in rows], *right]

    inv_radius = 1.0 / splat(radius_ref, 0)

    harm = [[column(part, var) for var in range(VARS)] for part in range(2)]
    left_mean, right_mean = [unpack_mean(packed) for packed in sides(H_ROWS, 8)]
    mean = []
    for var in range(VARS):
        own_mean = [load(mean_block, m_row(var, cell)) for cell in range(CELLS)]
        mean.append(
            left_mean[CELLS * var : CELLS * (var + 1)]
            + own_mean
            + right_mean[CELLS * var : CELLS * (var + 1)]
        )

    def smooth_parts(cells, at):
        center = cells[at]
        above, below = beside(center)
        diff_y = (above - below) * 0.5
        fourth = (
            (cells[at + 2] + cells[at - 2])
            + (up(center) + down(center))
            - 4.0 * ((cells[at + 1] + cells[at - 1]) + (above + below))
            + 12.0 * center
        )
        return diff_y, fourth

    harm_new = {}
    for cell in range(CELLS):
        at = 2 + cell
        wall = WALL_RATE * wall_ref[cell * C1 : (cell + 1) * C1, :]
        for part in range(2):
            diffs_x, diffs_y, fourths = [], [], []
            for var in range(VARS):
                cells = harm[part][var]
                diffs_x.append(
                    (mean[1][at + 1] * cells[at + 1] - mean[1][at - 1] * cells[at - 1]) * 0.5
                )
                diff_y, fourth = smooth_parts(cells, at)
                diffs_y.append(diff_y)
                fourths.append(fourth)
            flux_x = apply_matrix(0, diffs_x)
            flux_y = apply_matrix(VARS * VARS, diffs_y)
            for var in range(VARS):
                turned = omega * harm[1 - part][var][at]
                if part:
                    turned = -turned
                res = (
                    turned
                    - flux_x[var]
                    - flux_y[var]
                    - EPS_FOURTH * fourths[var]
                    - wall * harm[part][var][at]
                )
                row = h_row(part, var, cell)
                if stage:
                    res = h0_ref[row : row + C1, :] + step * res
                harm_new[part, var, cell] = res

    def stress(index, at):
        a, b = STRESS_PAIRS[index]
        return 0.5 * (harm[0][a][at] * harm[0][b][at] + harm[1][a][at] * harm[1][b][at])

    def total(tile):
        for shift in (4, 8, 16, 32, 64):
            tile = tile + pltpu.roll(tile, shift, 1)
        return jnp.take_along_axis(tile, lane % 4, axis=1)

    mean_new = {}
    for cell in range(CELLS):
        at = 2 + cell

        def grad_x(index):
            return (stress(index, at + 1) - stress(index, at - 1)) * 0.5

        def grad_y(tile):
            above, below = beside(tile)
            return (above - below) * 0.5

        s3, s4 = stress(3, at), stress(4, at)
        terms = [
            None,
            total(-grad_x(0) - grad_y(stress(1, at))),
            total(-grad_x(1) - grad_y(s3) - 2.0 * s4 * inv_radius),
            total(-grad_x(2) - grad_y(s4) + (s3 - stress(5, at)) * inv_radius),
            total(-grad_x(6) - grad_y(stress(7, at)) - stress(8, at) * inv_radius),
        ]
        diffs_x, diffs_y, fourths = [], [], []
        for var in range(VARS):
            cells = mean[var]
            diffs_x.append((cells[at + 1] - cells[at - 1]) * 0.5)
            diff_y, fourth = smooth_parts(cells, at)
            diffs_y.append(diff_y)
            fourths.append(fourth)
        flux_x = apply_matrix(0, diffs_x)
        flux_y = apply_matrix(VARS * VARS, diffs_y)
        for var in range(VARS):
            res = -flux_x[var] - flux_y[var] - EPS_FOURTH * fourths[var]
            if var:
                res = res + terms[var]
            row = m_row(var, cell)
            if stage:
                res = m0_ref[row : row + C1, :] + step * res
            mean_new[var, cell] = res

    if last:
        out_ref, rows_ref = outs
        target, offset = rows_ref, H_ROWS
    else:
        state_out, mean_out = outs
        target, offset = state_out, None
    for (part, var, cell), tile in harm_new.items():
        row = h_row(part, var, cell)
        target[row : row + C1, :] = tile
    for (var, cell), tile in mean_new.items():
        row = m_row(var, cell)
        if last:
            target[offset + row : offset + row + C1, :] = tile
        else:
            mean_out[row : row + C1, :] = tile
    if last:
        spare = H_ROWS + M_ROWS
        rows_ref[spare:, :] = jnp.zeros((rows_ref.shape[0] - spare, LANES), jnp.float32)
        turned = rows_ref[...].T
        for k in range(32):
            out_ref[k] = turned[4 * k : 4 * k + 4, :]
    else:
        state_out[H_ROWS:, :] = pack_mean(
            [mean_new[var, cell] for var in range(VARS) for cell in range(CELLS)]
        )


def restore_kernel(arrived_ref, mean_out, harm_out, rows_ref):
    for j in range(32):
        rows_ref[2 * j : 2 * j + 2, :] = arrived_ref[j, 0:2, :]
        rows_ref[NZ + 2 * j : NZ + 2 * j + 2, :] = arrived_ref[j, 2:4, :]
    turned = rows_ref[...].T
    for var in range(VARS):
        for cell in range(CELLS):
            for c1 in range(C1):
                cols = slice(c1 * LANES, (c1 + 1) * LANES)
                for part in range(2):
                    row = h_row(part, var, cell) + c1
                    harm_out[0, part, var, cell : cell + 1, cols] = turned[row : row + 1, :]
                row = H_ROWS + m_row(var, cell) + c1
                mean_out[var, cell : cell + 1, cols] = turned[row : row + 1, :]


def f32(*shape):
    return jax.ShapeDtypeStruct(shape, jnp.float32)


def kept(*shape):
    return pltpu.VMEM(shape, jnp.float32)


def held(*arrays):
    return [pltpu.with_memory_space_constraint(array, pltpu.VMEM) for array in arrays]


VMEM = pl.BlockSpec(memory_space=pltpu.VMEM)
SMEM = pl.BlockSpec(memory_space=pltpu.SMEM)


def rows_scratch(*shape):
    return [pltpu.VMEM(shape, jnp.float32)]


def shards(harmonics, mean_flow, freq_index, wall_mask, jacobian_x, jacobian_y):
    plane_count = mean_flow.shape[2]
    slab_count = lax.axis_size("slab")
    position = lax.axis_index("harm")

    sends, mean_start, wall, packed, speed, jac, radius = pl.pallas_call(
        open_kernel,
        out_shape=(
            kept(32, 4, 384),
            kept(M_ROWS, LANES),
            kept(W_ROWS, LANES),
            kept(8, LANES),
            kept(slab_count, 1, LANES),
            kept(2 * VARS * VARS, LANES),
            kept(8, LANES),
        ),
        in_specs=[VMEM] * 5 + [SMEM] * 2,
        out_specs=(VMEM,) * 7,
        scratch_shapes=rows_scratch(384, LANES) + rows_scratch(M_ROWS + W_ROWS, LANES),
        name="open",
    )(
        harmonics, mean_flow, wall_mask, jacobian_x, jacobian_y, freq_index,
        position.astype(jnp.int32).reshape(1),
    )
    arrived = lax.all_to_all(sends, "harm", 0, 0, tiled=True)
    start, omega = pl.pallas_call(
        unpack_kernel,
        out_shape=(kept(H_ROWS + 8, LANES), kept(8, LANES)),
        in_specs=[VMEM] * 2,
        out_specs=(VMEM,) * 2,
        scratch_shapes=rows_scratch(LANES, 384),
        name="unpack",
    )(*held(arrived, packed))

    omega, speed = lax.optimization_barrier((omega, speed))
    speeds = lax.all_to_all(speed, "slab", 0, 0, tiled=True)
    cell_count = CELLS * slab_count * plane_count

    core_pairs = [(i, i ^ 1) for i in range(slab_count)]
    chip_pairs = [
        pair for i in range(1, slab_count - 1, 2) for pair in ((i, i + 1), (i + 1, i))
    ]

    def beside(state):
        core = lax.ppermute(state, "slab", core_pairs)
        chip = lax.ppermute(state, "slab", chip_pairs)
        return state, core, chip

    def section(stage, *operands):
        if stage == len(SECTION_RATES) - 1:
            shapes, scratch = kept(32, 4, 512), rows_scratch(512, LANES)
            specs = VMEM
        else:
            shapes, scratch = (kept(H_ROWS + 8, LANES), kept(M_ROWS, LANES)), []
            specs = (VMEM, VMEM)
        return pl.pallas_call(
            functools.partial(section_kernel, stage=stage, cell_count=cell_count),
            out_shape=shapes,
            in_specs=[SMEM] + [VMEM] * len(operands),
            out_specs=specs,
            scratch_shapes=scratch,
        )(parity, *held(*operands))

    parity = (lax.axis_index("slab") % 2).astype(jnp.int32).reshape(1)
    fixed = (omega, wall, jac, radius)
    start_blocks = beside(start)
    residual, mean_residual = section(0, *start_blocks, mean_start, *fixed)
    state, mean_now = section(
        1, *start_blocks, mean_start, *fixed, speeds, *beside(residual), mean_residual
    )
    state, mean_now = section(2, *beside(state), mean_now, *fixed, speeds, start, mean_start)
    result = section(3, *beside(state), mean_now, *fixed, speeds, start, mean_start)
    back = lax.all_to_all(result, "harm", 0, 0, tiled=True)
    return pl.pallas_call(
        restore_kernel,
        out_shape=(f32(*mean_flow.shape), f32(*harmonics.shape)),
        in_specs=[VMEM],
        out_specs=(VMEM, VMEM),
        scratch_shapes=rows_scratch(LANES, 512),
        name="restore",
    )(*held(back))


def solution(mesh):
    placed = (
        P("harm", None, None, "slab", None),
        P(None, "slab", None),
        P("harm"),
        P("slab", None),
        P(),
        P(),
    )
    return jax.shard_map(
        shards,
        mesh=mesh,
        in_specs=placed,
        out_specs=(P(None, "slab", None), P("harm", None, None, "slab", None)),
        check_vma=False,
    )
```

```python
import functools

import jax
import jax.numpy as jnp
from jax import lax
from jax.experimental import pallas as pl
from jax.experimental.pallas import tpu as pltpu
from jax.sharding import PartitionSpec as P


NZ = 64
EPS_FOURTH = 0.05
COURANT = 0.9
OMEGA_BASE = 0.25
WALL_RATE = 2.0
HUB_RADIUS = 0.5
SECTION_RATES = (0.25, 1.0 / 3.0, 0.5, 1.0)
STRESS_PAIRS = ((1, 1), (1, 2), (1, 3), (2, 2), (2, 3), (3, 3), (4, 1), (4, 2), (4, 3))

VARS = 5
CELLS = 2
C1 = 16
LANES = 128
H_ROWS = 2 * VARS * CELLS * C1
M_ROWS = VARS * CELLS * C1
W_ROWS = CELLS * C1
F_END = H_ROWS + M_ROWS + 4 * CELLS * C1


def h_row(part, var, cell):
    return ((part * VARS + var) * CELLS + cell) * C1


def m_row(var, cell):
    return (var * CELLS + cell) * C1


def pack_mean(tiles):
    group = lax.broadcasted_iota(jnp.int32, (8, LANES), 1) // 4
    packed = jnp.zeros((8, LANES), jnp.float32)
    for i, tile in enumerate(tiles):
        for half in range(2):
            packed = jnp.where(group == 2 * i + half, tile[8 * half : 8 * half + 8, :], packed)
    return packed


def unpack_mean(packed):
    lane = lax.broadcasted_iota(jnp.int32, (8, LANES), 1) % 4
    tiles = []
    for i in range(VARS * CELLS):
        halves = [
            jnp.take_along_axis(packed, lane + 4 * (2 * i + half), axis=1) for half in range(2)
        ]
        tiles.append(jnp.concatenate(halves, axis=0))
    return tiles


def open_kernel(
    harm_ref, mean_ref, wall_ref, jac_x_ref, jac_y_ref, freq_ref, position_ref,
    out_ref, mean_out, wall_out, packed_out, speed_out, jac_out, radius_out,
    rows_ref, plane_ref
):
    for cell in range(CELLS):
        for c1 in range(C1):
            cols = slice(c1 * LANES, (c1 + 1) * LANES)
            for var in range(VARS):
                for part in range(2):
                    row = h_row(part, var, cell) + c1
                    rows_ref[row : row + 1, :] = harm_ref[0, part, var, cell : cell + 1, cols]
                row = m_row(var, cell) + c1
                plane_ref[row : row + 1, :] = mean_ref[var, cell : cell + 1, cols]
            row = M_ROWS + cell * C1 + c1
            plane_ref[row : row + 1, :] = wall_ref[cell : cell + 1, cols].astype(jnp.float32)
    omega = OMEGA_BASE * freq_ref[0].astype(jnp.float32)
    rows_ref[H_ROWS:, :] = jnp.full((rows_ref.shape[0] - H_ROWS, LANES), omega, jnp.float32)
    turned = rows_ref[...].T
    for j in range(32):
        out_ref[j, 0:2, :] = turned[2 * j : 2 * j + 2, :]
        out_ref[j, 2:4, :] = turned[NZ + 2 * j : NZ + 2 * j + 2, :]

    for base, matrix_ref in ((0, jac_x_ref), (VARS * VARS, jac_y_ref)):
        for a in range(VARS):
            for b in range(VARS):
                row = base + VARS * a + b
                jac_out[row : row + 1, :] = jnp.broadcast_to(
                    matrix_ref[a : a + 1, b : b + 1], (1, LANES)
                )
    lane = lax.broadcasted_iota(jnp.int32, (8, LANES), 1)
    radial = 2 * position_ref[0] + lane % 2
    radius_out[...] = HUB_RADIUS + (radial.astype(jnp.float32) + 0.5) / NZ
    source = ((lane // 2) % 2) * NZ + radial
    for start in range(0, M_ROWS + W_ROWS, 8):
        picked = jnp.take_along_axis(plane_ref[start : start + 8, :], source, axis=1)
        if start < M_ROWS:
            mean_out[start : start + 8, :] = picked
        else:
            wall_out[start - M_ROWS : start - M_ROWS + 8, :] = picked
    momentum = plane_ref[m_row(1, 0) : m_row(2, 0), :]
    speed_out[...] = jnp.full(speed_out.shape, jnp.sum(momentum * momentum), jnp.float32)
    packed_out[...] = pack_mean(
        [mean_out[i * C1 : (i + 1) * C1, :] for i in range(VARS * CELLS)]
    )


def unpack_kernel(arrived_ref, packed_ref, state_out, omega_out, rows_ref):
    for k in range(32):
        rows_ref[4 * k : 4 * k + 4, :] = arrived_ref[k]
    turned = rows_ref[...].T
    state_out[:H_ROWS, :] = turned[:H_ROWS, :]
    state_out[H_ROWS:, :] = packed_ref[...]
    omega_out[...] = turned[H_ROWS : H_ROWS + 8, :]


def tile_tools(jac_ref):
    lane = lax.broadcasted_iota(jnp.int32, (C1, LANES), 1)
    even = (lane // 2) % 2 == 0

    def up(tile):
        return pltpu.roll(tile, C1 - 1, 0)

    def down(tile):
        return pltpu.roll(tile, 1, 0)

    def beside(tile):
        swapped = jnp.where(even, pltpu.roll(tile, LANES - 2, 1), pltpu.roll(tile, 2, 1))
        return jnp.where(even, swapped, up(swapped)), jnp.where(even, down(swapped), swapped)

    def cross_parts(center):
        above, below = beside(center)
        fourth = (up(center) + down(center)) - 4.0 * (above + below) + 12.0 * center
        return (above - below) * 0.5, fourth

    def apply_matrix(base, tiles):
        out = []
        for a in range(VARS):
            total = splat(jac_ref, base + VARS * a) * tiles[0]
            for b in range(1, VARS):
                total = total + splat(jac_ref, base + VARS * a + b) * tiles[b]
            out.append(total)
        return out

    return lane, beside, cross_parts, apply_matrix


def splat(ref, row):
    return jnp.broadcast_to(ref[row : row + 1, :], (C1, LANES))


def time_step_of(speed_ref, cell_count):
    speed_total = jnp.sum(speed_ref[...], axis=0)
    time_step = COURANT / (1.0 + jnp.sqrt(speed_total / cell_count))
    return jnp.broadcast_to(time_step, (C1, LANES))


def load(block, row, first, count=C1):
    base, residual = block
    value = base[row : row + count, :]
    if residual is not None:
        value = value + first[:count] * residual[row : row + count, :]
    return value


def stress(left, right, index):
    a, b = STRESS_PAIRS[index]
    return 0.5 * (left[a] * left[b] + right[a] * right[b])


def own_terms(own, mean_block, first, omega_ref, wall_ref, jac_ref, radius_ref):
    _, beside, cross_parts, apply_matrix = tile_tools(jac_ref)
    omega = splat(omega_ref, 0)
    inv_radius = 1.0 / splat(radius_ref, 0)
    rows = {}
    for cell in range(CELLS):
        wall = WALL_RATE * wall_ref[cell * C1 : (cell + 1) * C1, :]
        harm = [
            [load(own, h_row(part, var, cell), first) for var in range(VARS)] for part in range(2)
        ]
        for part in range(2):
            diffs, fourths = zip(*[cross_parts(tile) for tile in harm[part]])
            flux = apply_matrix(VARS * VARS, diffs)
            for var in range(VARS):
                turned = omega * harm[1 - part][var]
                if part:
                    turned = -turned
                rows[h_row(part, var, cell)] = (
                    turned - flux[var] - EPS_FOURTH * fourths[var] - wall * harm[part][var]
                )
        mean = [load(mean_block, m_row(var, cell), first) for var in range(VARS)]
        diffs, fourths = zip(*[cross_parts(tile) for tile in mean])
        flux = apply_matrix(VARS * VARS, diffs)
        for var in range(VARS):
            rows[H_ROWS + m_row(var, cell)] = -flux[var] - EPS_FOURTH * fourths[var]

        def grad_y(tile):
            above, below = beside(tile)
            return (above - below) * 0.5

        s = [stress(*harm, index) for index in range(len(STRESS_PAIRS))]
        terms = [
            -grad_y(s[1]),
            -grad_y(s[3]) - 2.0 * s[4] * inv_radius,
            -grad_y(s[4]) + (s[3] - s[5]) * inv_radius,
            -grad_y(s[7]) - s[8] * inv_radius,
        ]
        for index, term in enumerate(terms):
            rows[f_row(index, cell)] = term
    return rows


def f_row(index, cell):
    return H_ROWS + M_ROWS + (index * CELLS + cell) * C1


def own_kernel(*refs, stage, cell_count):
    own_ref, mean_ref, omega_ref, wall_ref, jac_ref, radius_ref, *refs, out_ref = refs
    own, mean_block, first = (own_ref, None), (mean_ref, None), None
    if stage == 1:
        speed_ref, own_res, mean_res = refs
        first = SECTION_RATES[0] * time_step_of(speed_ref, cell_count)
        own, mean_block = (own_ref, own_res), (mean_ref, mean_res)
    rows = own_terms(own, mean_block, first, omega_ref, wall_ref, jac_ref, radius_ref)
    for row, tile in rows.items():
        out_ref[row : row + C1, :] = tile


def section_kernel(*refs, stage, cell_count):
    last = stage == len(SECTION_RATES) - 1
    parity_ref, own_ref, core_ref, chip_ref, mean_ref, *refs = refs
    own, core, chip = (own_ref, None), (core_ref, None), (chip_ref, None)
    mean_block, first = (mean_ref, None), None
    if stage == 0:
        omega_ref, wall_ref, jac_ref, radius_ref, *outs = refs
        near = own_terms(own, mean_block, first, omega_ref, wall_ref, jac_ref, radius_ref)
    else:
        jac_ref, near_ref, speed_ref, *refs = refs
        time_step = time_step_of(speed_ref, cell_count)
        step = SECTION_RATES[stage] * time_step
    if stage == 1:
        first = SECTION_RATES[0] * time_step
        own_res, core_res, chip_res, mean_res, *outs = refs
        own, core, chip = (own_ref, own_res), (core_ref, core_res), (chip_ref, chip_res)
        mean_block = (mean_ref, mean_res)
        h0_ref, m0_ref = own_ref, mean_ref
    elif stage:
        h0_ref, m0_ref, *outs = refs
    lane, _, _, apply_matrix = tile_tools(jac_ref)
    on_first = parity_ref[0] == 0

    def near_term(row):
        return near_ref[row : row + C1, :] if stage else near[row]

    def sides(row, count=C1):
        paired, other = load(core, row, first, count), load(chip, row, first, count)
        return jnp.where(on_first, other, paired), jnp.where(on_first, paired, other)

    def column(part, var):
        rows = [h_row(part, var, cell) for cell in range(CELLS)]
        left, right = zip(*[sides(row) for row in rows])
        return [*left, *[load(own, row, first) for row in rows], *right]

    harm = [[column(part, var) for var in range(VARS)] for part in range(2)]
    left_mean, right_mean = [unpack_mean(packed) for packed in sides(H_ROWS, 8)]
    mean = []
    for var in range(VARS):
        own_mean = [load(mean_block, m_row(var, cell), first) for cell in range(CELLS)]
        mean.append(
            left_mean[CELLS * var : CELLS * (var + 1)]
            + own_mean
            + right_mean[CELLS * var : CELLS * (var + 1)]
        )

    def axial_fourth(cells, at):
        return (cells[at + 2] + cells[at - 2]) - 4.0 * (cells[at + 1] + cells[at - 1])

    def total(tile):
        for shift in (4, 8, 16, 32, 64):
            tile = tile + pltpu.roll(tile, shift, 1)
        return jnp.take_along_axis(tile, lane % 4, axis=1)

    harm_new, mean_new = {}, {}
    for cell in range(CELLS):
        at = 2 + cell
        for part in range(2):
            diffs = [
                (mean[1][at + 1] * cells[at + 1] - mean[1][at - 1] * cells[at - 1]) * 0.5
                for cells in harm[part]
            ]
            flux = apply_matrix(0, diffs)
            for var in range(VARS):
                row = h_row(part, var, cell)
                res = near_term(row) - flux[var] - EPS_FOURTH * axial_fourth(harm[part][var], at)
                if stage:
                    res = h0_ref[row : row + C1, :] + step * res
                harm_new[part, var, cell] = res

        def grad_x(index):
            above, below = [
                stress(*[[cells[x] for cells in harm[part]] for part in range(2)], index)
                for x in (at + 1, at - 1)
            ]
            return (above - below) * 0.5

        terms = [
            total(near_term(f_row(i, cell)) - grad_x(index))
            for i, index in enumerate((0, 1, 2, 6))
        ]
        flux = apply_matrix(0, [(cells[at + 1] - cells[at - 1]) * 0.5 for cells in mean])
        for var in range(VARS):
            row = m_row(var, cell)
            res = near_term(H_ROWS + row) - flux[var] - EPS_FOURTH * axial_fourth(mean[var], at)
            if var:
                res = res + terms[var - 1]
            if stage:
                res = m0_ref[row : row + C1, :] + step * res
            mean_new[var, cell] = res

    if last:
        out_ref, rows_ref = outs
        target, offset = rows_ref, H_ROWS
    else:
        state_out, mean_out = outs
        target = state_out
    for (part, var, cell), tile in harm_new.items():
        row = h_row(part, var, cell)
        target[row : row + C1, :] = tile
    for (var, cell), tile in mean_new.items():
        row = m_row(var, cell)
        if last:
            target[offset + row : offset + row + C1, :] = tile
        else:
            mean_out[row : row + C1, :] = tile
    if last:
        spare = H_ROWS + M_ROWS
        rows_ref[spare:, :] = jnp.zeros((rows_ref.shape[0] - spare, LANES), jnp.float32)
        turned = rows_ref[...].T
        for k in range(32):
            out_ref[k] = turned[4 * k : 4 * k + 4, :]
    else:
        state_out[H_ROWS:, :] = pack_mean(
            [mean_new[var, cell] for var in range(VARS) for cell in range(CELLS)]
        )


def restore_kernel(arrived_ref, mean_out, harm_out, rows_ref):
    for j in range(32):
        rows_ref[2 * j : 2 * j + 2, :] = arrived_ref[j, 0:2, :]
        rows_ref[NZ + 2 * j : NZ + 2 * j + 2, :] = arrived_ref[j, 2:4, :]
    turned = rows_ref[...].T
    for var in range(VARS):
        for cell in range(CELLS):
            for c1 in range(C1):
                cols = slice(c1 * LANES, (c1 + 1) * LANES)
                for part in range(2):
                    row = h_row(part, var, cell) + c1
                    harm_out[0, part, var, cell : cell + 1, cols] = turned[row : row + 1, :]
                row = H_ROWS + m_row(var, cell) + c1
                mean_out[var, cell : cell + 1, cols] = turned[row : row + 1, :]


def f32(*shape):
    return jax.ShapeDtypeStruct(shape, jnp.float32)


def kept(*shape):
    return pltpu.VMEM(shape, jnp.float32)


def held(*arrays):
    return [pltpu.with_memory_space_constraint(array, pltpu.VMEM) for array in arrays]


VMEM = pl.BlockSpec(memory_space=pltpu.VMEM)
SMEM = pl.BlockSpec(memory_space=pltpu.SMEM)


def rows_scratch(*shape):
    return [pltpu.VMEM(shape, jnp.float32)]


def shards(harmonics, mean_flow, freq_index, wall_mask, jacobian_x, jacobian_y):
    plane_count = mean_flow.shape[2]
    slab_count = lax.axis_size("slab")
    position = lax.axis_index("harm")

    sends, mean_start, wall, packed, speed, jac, radius = pl.pallas_call(
        open_kernel,
        out_shape=(
            kept(32, 4, 384),
            kept(M_ROWS, LANES),
            kept(W_ROWS, LANES),
            kept(8, LANES),
            kept(slab_count, 1, LANES),
            kept(2 * VARS * VARS, LANES),
            kept(8, LANES),
        ),
        in_specs=[VMEM] * 5 + [SMEM] * 2,
        out_specs=(VMEM,) * 7,
        scratch_shapes=rows_scratch(384, LANES) + rows_scratch(M_ROWS + W_ROWS, LANES),
        name="open",
    )(
        harmonics, mean_flow, wall_mask, jacobian_x, jacobian_y, freq_index,
        position.astype(jnp.int32).reshape(1),
    )
    arrived = lax.all_to_all(sends, "harm", 0, 0, tiled=True)
    start, omega = pl.pallas_call(
        unpack_kernel,
        out_shape=(kept(H_ROWS + 8, LANES), kept(8, LANES)),
        in_specs=[VMEM] * 2,
        out_specs=(VMEM,) * 2,
        scratch_shapes=rows_scratch(LANES, 384),
        name="unpack",
    )(*held(arrived, packed))

    omega, speed = lax.optimization_barrier((omega, speed))
    speeds = lax.all_to_all(speed, "slab", 0, 0, tiled=True)
    cell_count = CELLS * slab_count * plane_count

    core_pairs = [(i, i ^ 1) for i in range(slab_count)]
    chip_pairs = [
        pair for i in range(1, slab_count - 1, 2) for pair in ((i, i + 1), (i + 1, i))
    ]

    def beside(state):
        core = lax.ppermute(state, "slab", core_pairs)
        chip = lax.ppermute(state, "slab", chip_pairs)
        return state, core, chip

    def section(stage, *operands):
        if stage == len(SECTION_RATES) - 1:
            shapes, scratch = kept(32, 4, 512), rows_scratch(512, LANES)
            specs = VMEM
        else:
            shapes, scratch = (kept(H_ROWS + 8, LANES), kept(M_ROWS, LANES)), []
            specs = (VMEM, VMEM)
        return pl.pallas_call(
            functools.partial(section_kernel, stage=stage, cell_count=cell_count),
            out_shape=shapes,
            in_specs=[SMEM] + [VMEM] * len(operands),
            out_specs=specs,
            scratch_shapes=scratch,
        )(parity, *held(*operands))

    def own_part(stage, *operands):
        return pl.pallas_call(
            functools.partial(own_kernel, stage=stage, cell_count=cell_count),
            out_shape=[kept(F_END, LANES)],
            in_specs=[VMEM] * len(operands),
            out_specs=[VMEM],
        )(*held(*operands))

    parity = (lax.axis_index("slab") % 2).astype(jnp.int32).reshape(1)
    fixed = (omega, wall, jac, radius)
    blocks = beside(start)
    residual, mean_residual = section(0, *blocks, mean_start, *fixed)
    residual_blocks = beside(residual)
    (near,) = own_part(1, start, mean_start, *fixed, speeds, residual, mean_residual)
    state, mean_now = section(
        1, *blocks, mean_start, jac, near, speeds, *residual_blocks, mean_residual
    )
    blocks = beside(state)
    (near,) = own_part(2, state, mean_now, *fixed)
    state, mean_now = section(
        2, *blocks, mean_now, jac, near, speeds, start, mean_start
    )
    blocks = beside(state)
    (near,) = own_part(3, state, mean_now, *fixed)
    result = section(3, *blocks, mean_now, jac, near, speeds, start, mean_start)
    back = lax.all_to_all(result, "harm", 0, 0, tiled=True)
    return pl.pallas_call(
        restore_kernel,
        out_shape=(f32(*mean_flow.shape), f32(*harmonics.shape)),
        in_specs=[VMEM],
        out_specs=(VMEM, VMEM),
        scratch_shapes=rows_scratch(LANES, 512),
        name="restore",
    )(*held(back))


def solution(mesh):
    placed = (
        P("harm", None, None, "slab", None),
        P(None, "slab", None),
        P("harm"),
        P("slab", None),
        P(),
        P(),
    )
    return jax.shard_map(
        shards,
        mesh=mesh,
        in_specs=placed,
        out_specs=(P(None, "slab", None), P("harm", None, None, "slab", None)),
        check_vma=False,
    )
```

```python
import functools

import jax
import jax.numpy as jnp
from jax import lax
from jax.experimental import pallas as pl
from jax.experimental.pallas import tpu as pltpu
from jax.sharding import PartitionSpec as P


NZ = 64
EPS_FOURTH = 0.05
COURANT = 0.9
OMEGA_BASE = 0.25
WALL_RATE = 2.0
HUB_RADIUS = 0.5
SECTION_RATES = (0.25, 1.0 / 3.0, 0.5, 1.0)
STRESS_PAIRS = ((1, 1), (1, 2), (1, 3), (2, 2), (2, 3), (3, 3), (4, 1), (4, 2), (4, 3))

VARS = 5
CELLS = 2
C1 = 16
LANES = 128
H_ROWS = 2 * VARS * CELLS * C1
M_ROWS = VARS * CELLS * C1
W_ROWS = CELLS * C1
F_END = H_ROWS + M_ROWS + 4 * CELLS * C1


def h_row(part, var, cell):
    return ((part * VARS + var) * CELLS + cell) * C1


def m_row(var, cell):
    return (var * CELLS + cell) * C1


def pack_mean(tiles):
    group = lax.broadcasted_iota(jnp.int32, (8, LANES), 1) // 4
    packed = jnp.zeros((8, LANES), jnp.float32)
    for i, tile in enumerate(tiles):
        for half in range(2):
            packed = jnp.where(group == 2 * i + half, tile[8 * half : 8 * half + 8, :], packed)
    return packed


def unpack_mean(packed):
    lane = lax.broadcasted_iota(jnp.int32, (8, LANES), 1) % 4
    tiles = []
    for i in range(VARS * CELLS):
        halves = [
            jnp.take_along_axis(packed, lane + 4 * (2 * i + half), axis=1) for half in range(2)
        ]
        tiles.append(jnp.concatenate(halves, axis=0))
    return tiles


def open_kernel(
    harm_ref, mean_ref, wall_ref, jac_x_ref, jac_y_ref, freq_ref, position_ref,
    out_ref, mean_out, wall_out, packed_out, speed_out, jac_out, radius_out,
    rows_ref, plane_ref
):
    for c1 in range(C1):
        cols = slice(c1 * LANES, (c1 + 1) * LANES)
        for var in range(VARS):
            for part in range(2):
                pair = harm_ref[0, part, var, :, cols]
                for cell in range(CELLS):
                    row = h_row(part, var, cell) + c1
                    rows_ref[row : row + 1, :] = pair[cell : cell + 1, :]
            pair = mean_ref[var, :, cols]
            for cell in range(CELLS):
                row = m_row(var, cell) + c1
                plane_ref[row : row + 1, :] = pair[cell : cell + 1, :]
        pair = wall_ref[:, cols].astype(jnp.float32)
        for cell in range(CELLS):
            row = M_ROWS + cell * C1 + c1
            plane_ref[row : row + 1, :] = pair[cell : cell + 1, :]
    omega = OMEGA_BASE * freq_ref[0].astype(jnp.float32)
    rows_ref[H_ROWS:, :] = jnp.full((rows_ref.shape[0] - H_ROWS, LANES), omega, jnp.float32)
    turned = rows_ref[...].T
    for j in range(32):
        out_ref[j, 0:2, :] = turned[2 * j : 2 * j + 2, :]
        out_ref[j, 2:4, :] = turned[NZ + 2 * j : NZ + 2 * j + 2, :]

    for base, matrix_ref in ((0, jac_x_ref), (VARS * VARS, jac_y_ref)):
        for a in range(VARS):
            for b in range(VARS):
                row = base + VARS * a + b
                jac_out[row : row + 1, :] = 0.5 * jnp.broadcast_to(
                    matrix_ref[a : a + 1, b : b + 1], (1, LANES)
                )
    lane = lax.broadcasted_iota(jnp.int32, (8, LANES), 1)
    radial = 2 * position_ref[0] + lane % 2
    radius_out[...] = HUB_RADIUS + (radial.astype(jnp.float32) + 0.5) / NZ
    source = ((lane // 2) % 2) * NZ + radial
    for start in range(0, M_ROWS + W_ROWS, 8):
        picked = jnp.take_along_axis(plane_ref[start : start + 8, :], source, axis=1)
        if start < M_ROWS:
            mean_out[start : start + 8, :] = picked
        else:
            wall_out[start - M_ROWS : start - M_ROWS + 8, :] = picked
    momentum = plane_ref[m_row(1, 0) : m_row(2, 0), :]
    speed_out[...] = jnp.full(speed_out.shape, jnp.sum(momentum * momentum), jnp.float32)
    packed_out[...] = pack_mean(
        [mean_out[i * C1 : (i + 1) * C1, :] for i in range(VARS * CELLS)]
    )


def unpack_kernel(arrived_ref, packed_ref, state_out, omega_out, rows_ref):
    for k in range(32):
        rows_ref[4 * k : 4 * k + 4, :] = arrived_ref[k]
    turned = rows_ref[...].T
    state_out[:H_ROWS, :] = turned[:H_ROWS, :]
    state_out[H_ROWS:, :] = packed_ref[...]
    omega_out[...] = turned[H_ROWS : H_ROWS + 8, :]


def tile_tools(jac_ref):
    lane = lax.broadcasted_iota(jnp.int32, (C1, LANES), 1)
    even = (lane // 2) % 2 == 0

    def up(tile):
        return pltpu.roll(tile, C1 - 1, 0)

    def down(tile):
        return pltpu.roll(tile, 1, 0)

    def beside(tile):
        swapped = jnp.where(even, pltpu.roll(tile, LANES - 2, 1), pltpu.roll(tile, 2, 1))
        return jnp.where(even, swapped, up(swapped)), jnp.where(even, down(swapped), swapped)

    def cross_parts(center):
        above, below = beside(center)
        fourth = (up(center) + down(center)) - 4.0 * (above + below) + 12.0 * center
        return above - below, fourth

    def apply_matrix(base, tiles):
        out = []
        for a in range(VARS):
            total = splat(jac_ref, base + VARS * a) * tiles[0]
            for b in range(1, VARS):
                total = total + splat(jac_ref, base + VARS * a + b) * tiles[b]
            out.append(total)
        return out

    return lane, beside, cross_parts, apply_matrix


def splat(ref, row):
    return jnp.broadcast_to(ref[row : row + 1, :], (C1, LANES))


def time_step_of(speed_ref, cell_count):
    speed_total = jnp.sum(speed_ref[...], axis=0)
    time_step = COURANT / (1.0 + jnp.sqrt(speed_total / cell_count))
    return jnp.broadcast_to(time_step, (C1, LANES))


def load(block, row, first, count=C1):
    base, residual = block
    value = base[row : row + count, :]
    if residual is not None:
        value = value + first[:count] * residual[row : row + count, :]
    return value


def stress(left, right, index):
    a, b = STRESS_PAIRS[index]
    return left[a] * left[b] + right[a] * right[b]


def own_terms(own, mean_block, first, omega_ref, wall_ref, jac_ref, radius_ref):
    _, beside, cross_parts, apply_matrix = tile_tools(jac_ref)
    omega = splat(omega_ref, 0)
    half_inv_radius = 0.5 / splat(radius_ref, 0)
    rows = {}
    for cell in range(CELLS):
        wall = WALL_RATE * wall_ref[cell * C1 : (cell + 1) * C1, :]
        harm = [
            [load(own, h_row(part, var, cell), first) for var in range(VARS)] for part in range(2)
        ]
        for part in range(2):
            diffs, fourths = zip(*[cross_parts(tile) for tile in harm[part]])
            flux = apply_matrix(VARS * VARS, diffs)
            for var in range(VARS):
                turned = omega * harm[1 - part][var]
                if part:
                    turned = -turned
                rows[h_row(part, var, cell)] = (
                    turned - flux[var] - EPS_FOURTH * fourths[var] - wall * harm[part][var]
                )
        mean = [load(mean_block, m_row(var, cell), first) for var in range(VARS)]
        diffs, fourths = zip(*[cross_parts(tile) for tile in mean])
        flux = apply_matrix(VARS * VARS, diffs)
        for var in range(VARS):
            rows[H_ROWS + m_row(var, cell)] = -flux[var] - EPS_FOURTH * fourths[var]

        def grad_y(tile):
            above, below = beside(tile)
            return (above - below) * 0.25

        s = [stress(*harm, index) for index in range(len(STRESS_PAIRS))]
        terms = [
            -grad_y(s[1]),
            -grad_y(s[3]) - 2.0 * s[4] * half_inv_radius,
            -grad_y(s[4]) + (s[3] - s[5]) * half_inv_radius,
            -grad_y(s[7]) - s[8] * half_inv_radius,
        ]
        for index, term in enumerate(terms):
            rows[f_row(index, cell)] = term
    return rows


def f_row(index, cell):
    return H_ROWS + M_ROWS + (index * CELLS + cell) * C1


def own_kernel(*refs, stage, cell_count):
    own_ref, mean_ref, omega_ref, wall_ref, jac_ref, radius_ref, *refs, out_ref = refs
    own, mean_block, first = (own_ref, None), (mean_ref, None), None
    if stage == 1:
        speed_ref, own_res, mean_res = refs
        first = SECTION_RATES[0] * time_step_of(speed_ref, cell_count)
        own, mean_block = (own_ref, own_res), (mean_ref, mean_res)
    rows = own_terms(own, mean_block, first, omega_ref, wall_ref, jac_ref, radius_ref)
    for row, tile in rows.items():
        out_ref[row : row + C1, :] = tile


def section_kernel(*refs, stage, cell_count):
    last = stage == len(SECTION_RATES) - 1
    parity_ref, own_ref, core_ref, chip_ref, mean_ref, *refs = refs
    own, core, chip = (own_ref, None), (core_ref, None), (chip_ref, None)
    mean_block, first = (mean_ref, None), None
    if stage == 0:
        omega_ref, wall_ref, jac_ref, radius_ref, *outs = refs
        near = own_terms(own, mean_block, first, omega_ref, wall_ref, jac_ref, radius_ref)
    else:
        jac_ref, near_ref, speed_ref, *refs = refs
        time_step = time_step_of(speed_ref, cell_count)
        step = SECTION_RATES[stage] * time_step
    if stage == 1:
        first = SECTION_RATES[0] * time_step
        own_res, core_res, chip_res, mean_res, *outs = refs
        own, core, chip = (own_ref, own_res), (core_ref, core_res), (chip_ref, chip_res)
        mean_block = (mean_ref, mean_res)
        h0_ref, m0_ref = own_ref, mean_ref
    elif stage:
        h0_ref, m0_ref, *outs = refs
    lane, _, _, apply_matrix = tile_tools(jac_ref)
    on_first = parity_ref[0] == 0

    def near_term(row):
        return near_ref[row : row + C1, :] if stage else near[row]

    def sides(row, count=C1):
        paired, other = load(core, row, first, count), load(chip, row, first, count)
        return jnp.where(on_first, other, paired), jnp.where(on_first, paired, other)

    def column(part, var):
        rows = [h_row(part, var, cell) for cell in range(CELLS)]
        left, right = zip(*[sides(row) for row in rows])
        return [*left, *[load(own, row, first) for row in rows], *right]

    harm = [[column(part, var) for var in range(VARS)] for part in range(2)]
    left_mean, right_mean = [unpack_mean(packed) for packed in sides(H_ROWS, 8)]
    mean = []
    for var in range(VARS):
        own_mean = [load(mean_block, m_row(var, cell), first) for cell in range(CELLS)]
        mean.append(
            left_mean[CELLS * var : CELLS * (var + 1)]
            + own_mean
            + right_mean[CELLS * var : CELLS * (var + 1)]
        )

    def axial_fourth(cells, at):
        return (cells[at + 2] + cells[at - 2]) - 4.0 * (cells[at + 1] + cells[at - 1])

    def total(tile):
        for shift in (4, 8, 16, 32, 64):
            tile = tile + pltpu.roll(tile, shift, 1)
        return jnp.take_along_axis(tile, lane % 4, axis=1)

    harm_new, mean_new = {}, {}
    for cell in range(CELLS):
        at = 2 + cell
        for part in range(2):
            diffs = [
                mean[1][at + 1] * cells[at + 1] - mean[1][at - 1] * cells[at - 1]
                for cells in harm[part]
            ]
            flux = apply_matrix(0, diffs)
            for var in range(VARS):
                row = h_row(part, var, cell)
                res = near_term(row) - flux[var] - EPS_FOURTH * axial_fourth(harm[part][var], at)
                if stage:
                    res = h0_ref[row : row + C1, :] + step * res
                harm_new[part, var, cell] = res

        def grad_x(index):
            above, below = [
                stress(*[[cells[x] for cells in harm[part]] for part in range(2)], index)
                for x in (at + 1, at - 1)
            ]
            return (above - below) * 0.25

        terms = [
            total(near_term(f_row(i, cell)) - grad_x(index))
            for i, index in enumerate((0, 1, 2, 6))
        ]
        flux = apply_matrix(0, [cells[at + 1] - cells[at - 1] for cells in mean])
        for var in range(VARS):
            row = m_row(var, cell)
            res = near_term(H_ROWS + row) - flux[var] - EPS_FOURTH * axial_fourth(mean[var], at)
            if var:
                res = res + terms[var - 1]
            if stage:
                res = m0_ref[row : row + C1, :] + step * res
            mean_new[var, cell] = res

    if last:
        out_ref, rows_ref = outs
        target, offset = rows_ref, H_ROWS
    else:
        state_out, mean_out = outs
        target = state_out
    for (part, var, cell), tile in harm_new.items():
        row = h_row(part, var, cell)
        target[row : row + C1, :] = tile
    for (var, cell), tile in mean_new.items():
        row = m_row(var, cell)
        if last:
            target[offset + row : offset + row + C1, :] = tile
        else:
            mean_out[row : row + C1, :] = tile
    if last:
        spare = H_ROWS + M_ROWS
        rows_ref[spare:, :] = jnp.zeros((rows_ref.shape[0] - spare, LANES), jnp.float32)
        turned = rows_ref[...].T
        for k in range(32):
            out_ref[k] = turned[4 * k : 4 * k + 4, :]
    else:
        state_out[H_ROWS:, :] = pack_mean(
            [mean_new[var, cell] for var in range(VARS) for cell in range(CELLS)]
        )


def restore_kernel(arrived_ref, mean_out, harm_out, rows_ref):
    for j in range(32):
        rows_ref[2 * j : 2 * j + 2, :] = arrived_ref[j, 0:2, :]
        rows_ref[NZ + 2 * j : NZ + 2 * j + 2, :] = arrived_ref[j, 2:4, :]
    turned = rows_ref[...].T

    def pair(rows):
        return jnp.concatenate([turned[row : row + 1, :] for row in rows], axis=0)

    for var in range(VARS):
        for c1 in range(C1):
            cols = slice(c1 * LANES, (c1 + 1) * LANES)
            for part in range(2):
                harm_out[0, part, var, :, cols] = pair(
                    [h_row(part, var, cell) + c1 for cell in range(CELLS)]
                )
            mean_out[var, :, cols] = pair(
                [H_ROWS + m_row(var, cell) + c1 for cell in range(CELLS)]
            )


def f32(*shape):
    return jax.ShapeDtypeStruct(shape, jnp.float32)


def kept(*shape):
    return pltpu.VMEM(shape, jnp.float32)


def held(*arrays):
    return [pltpu.with_memory_space_constraint(array, pltpu.VMEM) for array in arrays]


VMEM = pl.BlockSpec(memory_space=pltpu.VMEM)
SMEM = pl.BlockSpec(memory_space=pltpu.SMEM)


def rows_scratch(*shape):
    return [pltpu.VMEM(shape, jnp.float32)]


def shards(harmonics, mean_flow, freq_index, wall_mask, jacobian_x, jacobian_y):
    plane_count = mean_flow.shape[2]
    slab_count = lax.axis_size("slab")
    position = lax.axis_index("harm")

    sends, mean_start, wall, packed, speed, jac, radius = pl.pallas_call(
        open_kernel,
        out_shape=(
            kept(32, 4, 384),
            kept(M_ROWS, LANES),
            kept(W_ROWS, LANES),
            kept(8, LANES),
            kept(slab_count, 1, LANES),
            kept(2 * VARS * VARS, LANES),
            kept(8, LANES),
        ),
        in_specs=[VMEM] * 5 + [SMEM] * 2,
        out_specs=(VMEM,) * 7,
        scratch_shapes=rows_scratch(384, LANES) + rows_scratch(M_ROWS + W_ROWS, LANES),
        name="open",
    )(
        harmonics, mean_flow, wall_mask, jacobian_x, jacobian_y, freq_index,
        position.astype(jnp.int32).reshape(1),
    )
    arrived = lax.all_to_all(sends, "harm", 0, 0, tiled=True)
    start, omega = pl.pallas_call(
        unpack_kernel,
        out_shape=(kept(H_ROWS + 8, LANES), kept(8, LANES)),
        in_specs=[VMEM] * 2,
        out_specs=(VMEM,) * 2,
        scratch_shapes=rows_scratch(LANES, 384),
        name="unpack",
    )(*held(arrived, packed))

    omega, speed = lax.optimization_barrier((omega, speed))
    speeds = lax.all_to_all(speed, "slab", 0, 0, tiled=True)
    cell_count = CELLS * slab_count * plane_count

    core_pairs = [(i, i ^ 1) for i in range(slab_count)]
    chip_pairs = [
        pair for i in range(1, slab_count - 1, 2) for pair in ((i, i + 1), (i + 1, i))
    ]

    def beside(state):
        core = lax.ppermute(state, "slab", core_pairs)
        chip = lax.ppermute(state, "slab", chip_pairs)
        return state, core, chip

    def section(stage, *operands):
        if stage == len(SECTION_RATES) - 1:
            shapes, scratch = kept(32, 4, 512), rows_scratch(512, LANES)
            specs = VMEM
        else:
            shapes, scratch = (kept(H_ROWS + 8, LANES), kept(M_ROWS, LANES)), []
            specs = (VMEM, VMEM)
        return pl.pallas_call(
            functools.partial(section_kernel, stage=stage, cell_count=cell_count),
            out_shape=shapes,
            in_specs=[SMEM] + [VMEM] * len(operands),
            out_specs=specs,
            scratch_shapes=scratch,
        )(parity, *held(*operands))

    def own_part(stage, *operands):
        return pl.pallas_call(
            functools.partial(own_kernel, stage=stage, cell_count=cell_count),
            out_shape=[kept(F_END, LANES)],
            in_specs=[VMEM] * len(operands),
            out_specs=[VMEM],
        )(*held(*operands))

    parity = (lax.axis_index("slab") % 2).astype(jnp.int32).reshape(1)
    fixed = (omega, wall, jac, radius)
    blocks = beside(start)
    residual, mean_residual = section(0, *blocks, mean_start, *fixed)
    residual_blocks = beside(residual)
    (near,) = own_part(1, start, mean_start, *fixed, speeds, residual, mean_residual)
    state, mean_now = section(
        1, *blocks, mean_start, jac, near, speeds, *residual_blocks, mean_residual
    )
    blocks = beside(state)
    (near,) = own_part(2, state, mean_now, *fixed)
    state, mean_now = section(
        2, *blocks, mean_now, jac, near, speeds, start, mean_start
    )
    blocks = beside(state)
    (near,) = own_part(3, state, mean_now, *fixed)
    result = section(3, *blocks, mean_now, jac, near, speeds, start, mean_start)
    back = lax.all_to_all(result, "harm", 0, 0, tiled=True)
    return pl.pallas_call(
        restore_kernel,
        out_shape=(f32(*mean_flow.shape), f32(*harmonics.shape)),
        in_specs=[VMEM],
        out_specs=(VMEM, VMEM),
        scratch_shapes=rows_scratch(LANES, 512),
        name="restore",
    )(*held(back))


def solution(mesh):
    placed = (
        P("harm", None, None, "slab", None),
        P(None, "slab", None),
        P("harm"),
        P("slab", None),
        P(),
        P(),
    )
    return jax.shard_map(
        shards,
        mesh=mesh,
        in_specs=placed,
        out_specs=(P(None, "slab", None), P("harm", None, None, "slab", None)),
        check_vma=False,
    )
```
